256 devices in a mesh: dp: 32 (over y, x, core), tensor: 8 (over z).
Axes of the slice: x: 4, y: 4, z: 8, core: 2. Of those that a mesh axis runs over, the one named last changes fastest.
Arguments:
- frames: bfloat16 [8192, 4, 84, 84], P(('dp', 'tensor')), may hold values from 0 to 1
- counts: int32 [8, 32], replicated, may hold values from 1 to 32, 512 in all within a row
- slot_ids: int32 [32, 128], P('dp'), may hold values from 0 to 255, as said below
- reset_flags: int32 [32, 256], P('dp'), may hold values 0 or 1
- hidden_state: float32 [2048, 8192], P('tensor', 'dp'), may hold values from -1 to 1
- cell_state: float32 [2048, 8192], P('tensor', 'dp'), may hold values from -6 to 6
- conv_first: bfloat16 [16, 4, 3, 3], replicated, may hold values from -1.5 to 1.5
- conv_second: bfloat16 [32, 16, 3, 3], replicated, may hold values from -0.75 to 0.75
- conv_third: bfloat16 [32, 32, 3, 3], replicated, may hold values from -0.5 to 0.5
- res_first: bfloat16 [32, 32, 3, 3], replicated, may hold values from -0.5 to 0.5
- res_second: bfloat16 [32, 32, 3, 3], replicated, may hold values from -0.5 to 0.5
- projection: bfloat16 [256, 3872], replicated, may hold values from -0.125 to 0.125
- input_weight: bfloat16 [4, 2048, 256], P(None, 'tensor'), may hold values from -0.375 to 0.375
- recur_weight: bfloat16 [4, 2048, 2048], P(None, 'tensor'), may hold values from -0.125 to 0.125
- gate_bias: float32 [4, 2048], P(None, 'tensor'), may hold values from -3 to 3
- head_weight: bfloat16 [19, 2048], P(None, 'tensor'), may hold values from -0.125 to 0.125
Outputs:
- policy_out: float32 [19, 8192], P(None, ('dp', 'tensor'))
- hidden_after: float32 [2048, 8192], P('tensor', 'dp')
- cell_after: float32 [2048, 8192], P('tensor', 'dp')
The draws below stay inside these ranges and needn't reach their ends.
Inputs may be any that keep to these rules, and one draw needn't show every extreme that they name: Arrival rows fill the first counts[t, a] slots of their device; each row of counts sums to 512. `slot_ids`: the entries of one dp index are distinct.
All inputs are finite; a program needn't handle non-finite values. No bound on the sum of `reset_flags` on one device may be relied on, other than what follows from the above.
Results may differ from the reference program's by a relative error of at most 0.008.
Values may be sent and summed in bfloat16 or wider, within the bound.
A program may use at most 128 MiB of HBM per device.

```python
import math
import jax
import jax.numpy as jnp
import numpy as np
from jax import lax

STACK = 4
FRAME = 84
C1 = 16
C2 = 32
FLAT = 3872
FEAT = 256
H = 2048
ACTIONS = 18
ROWS_DEV = 16
CAP = 32
ROWS_GRP = 128
SLOTS = 256
ARRIVE = 8192
N_DP = 32
N_TENSOR = 8


def draw_slot_ids(key, part):
    keys = jax.random.split(jax.random.fold_in(key, 17), N_DP)

    def one_group(group_key):
        return jax.random.permutation(group_key, SLOTS)[:ROWS_GRP].astype(jnp.int32)
    return jax.vmap(one_group)(keys)


def place_ends(entries, own_key, least, largest):
    longest = entries.shape.index(max(entries.shape))
    spots = []
    for shift in (0, 1):
        where = [jax.random.randint(jax.random.fold_in(own_key, axis), (), 0, length) for axis, length in enumerate(entries.shape)]
        where[longest] = (where[longest] + shift) % entries.shape[longest]
        spots.append(tuple(where))
    return entries.at[spots[0]].set(least).at[spots[1]].set(largest)


def block_scale(rng, extent, pieces, smallest, largest):
    loudness, own = 1.0, jax.random.fold_in(rng, 6)
    for dim, shards_of in pieces:
        heights = jnp.exp(jax.random.uniform(jax.random.fold_in(own, dim), (shards_of,), jnp.float32, smallest / len(pieces), largest / len(pieces)))
        loudness = loudness * jnp.repeat(heights, extent[dim] // shards_of).reshape([-1 if axis == dim else 1 for axis in range(len(extent))])
    return loudness


def length_profile(amount, total, limit, skew):
    weights = [(1 << 20) // math.isqrt(grade ** skew) + 1 for grade in range(2, amount + 1)]
    surplus, holding = total - limit - (amount - 1), [1] * (amount - 1)
    while surplus > 0:
        movable = [i for i in range(amount - 1) if holding[i] < limit]
        mass, left = sum([weights[i] for i in movable]), surplus
        for i in movable:
            addition = min(limit - holding[i], max(1, left * weights[i] // mass), surplus)
            holding[i] = holding[i] + addition
            surplus = surplus - addition
    return np.array([limit] + holding)


def ragged_sizes(stream_key, number_of, total, most, lean):
    if number_of == 2:
        one = jax.random.randint(stream_key, (), max(1, total - most), min(most, total - 1) + 1)
        return jnp.stack([one, total - one])
    tallies = jnp.asarray(length_profile(number_of, total, most, lean), jnp.int32)
    twos = (number_of - 1) // 2
    giver, taker = tallies[1:1 + 2 * twos:2], tallies[2:2 + 2 * twos:2]
    slack = jnp.minimum(giver - 1, most - taker)
    moved = jax.random.randint(jax.random.fold_in(stream_key, 1), (twos,), 0, 1 << 20) % (slack + 1)
    tallies = tallies.at[1:1 + 2 * twos:2].set(giver - moved).at[2:2 + 2 * twos:2].set(taker + moved)
    return tallies[jax.random.permutation(jax.random.fold_in(stream_key, 2), number_of)]


def gaussian(key, extent, scale, limit, pieces=(), kind=jnp.bfloat16):
    loudness = block_scale(key, extent, pieces, -0.22, 0.18) if pieces else 1.0
    array = jax.random.normal(key, extent, jnp.float32) * scale * loudness
    return jnp.minimum(jnp.maximum(array, -limit), limit).astype(kind)


def setup_inputs(seed: int = 0) -> dict:
    key_list = jax.random.split(jax.random.key(seed), 17)
    return {
        "frames": jnp.clip(1.0 * jax.random.uniform(key_list[0], (ARRIVE, STACK, FRAME, FRAME), jnp.float32) ** block_scale(key_list[0], (ARRIVE, STACK, FRAME, FRAME), ((0, 256),), -0.2, 0.2), 0.0, 1.0).astype(jnp.bfloat16),
        "counts": jax.vmap(lambda own: ragged_sizes(own, N_DP, ROWS_DEV * N_DP, CAP, 2))(jax.random.split(key_list[1], N_TENSOR)).reshape((N_TENSOR, N_DP)).astype(jnp.int32),
        "slot_ids": draw_slot_ids(jax.random.fold_in(key_list[16], 71), 0),
        "reset_flags": place_ends((jax.random.randint(key_list[3], (N_DP, SLOTS), 0, 4) < 1).astype(jnp.int32), jax.random.fold_in(key_list[3], 1), 0, 1),
        "hidden_state": jnp.clip(jax.random.uniform(key_list[4], (H, N_DP * SLOTS), jnp.float32, -1.0, 1.0) * block_scale(key_list[4], (H, N_DP * SLOTS), ((0, 8), (1, 32)), -0.4, 0.0), -1.0, 1.0),
        "cell_state": gaussian(key_list[5], (H, N_DP * SLOTS), 1.0, 6.0, ((0, 8), (1, 32)), jnp.float32),
        "conv_first": gaussian(key_list[6], (C1, STACK, 3, 3), 18 ** -0.5, 1.5),
        "conv_second": gaussian(key_list[7], (C2, C1, 3, 3), 72 ** -0.5, 0.75),
        "conv_third": gaussian(key_list[8], (C2, C2, 3, 3), 144 ** -0.5, 0.5),
        "res_first": gaussian(key_list[9], (C2, C2, 3, 3), 144 ** -0.5, 0.5),
        "res_second": gaussian(key_list[10], (C2, C2, 3, 3), 144 ** -0.5, 0.5),
        "projection": gaussian(key_list[11], (FEAT, FLAT), (FLAT // 2) ** -0.5, 0.125),
        "input_weight": gaussian(key_list[12], (4, H, FEAT), FEAT ** -0.5, 0.375, ((1, 8),)),
        "recur_weight": gaussian(key_list[13], (4, H, H), H ** -0.5, 0.125, ((1, 8),)),
        "gate_bias": gaussian(key_list[14], (4, H), 0.5, 3.0, ((1, 8),), jnp.float32),
        "head_weight": gaussian(key_list[15], (ACTIONS + 1, H), H ** -0.5, 0.125, ((1, 8),)),
    }


def rounded(values):
    return lax.optimization_barrier(values.astype(jnp.bfloat16)).astype(jnp.float32)


def conv_same(inputs, kernel):
    return lax.conv_general_dilated(inputs, kernel.astype(jnp.float32), (1, 1), "SAME", dimension_numbers=("NCHW", "OIHW", "NCHW"), precision=lax.Precision.HIGHEST)


def pooled(inputs):
    return lax.reduce_window(inputs, -jnp.inf, lax.max, (1, 1, 3, 3), (1, 1, 2, 2), "SAME")


def encode(images, conv_first, conv_second, conv_third, res_first, res_second, projection):
    section_one = rounded(jax.nn.relu(pooled(conv_same(images.astype(jnp.float32), conv_first))))
    section_two = rounded(jax.nn.relu(pooled(conv_same(section_one, conv_second))))
    section_three = rounded(pooled(conv_same(section_two, conv_third)))
    residual_in = rounded(jax.nn.relu(conv_same(jax.nn.relu(section_three), res_first)))
    encoded_map = rounded(jax.nn.relu(section_three + conv_same(residual_in, res_second)))
    flattened = encoded_map.reshape(encoded_map.shape[0], -1)
    product = lax.dot_general(projection.astype(jnp.float32), flattened, (((1,), (1,)), ((), ())), precision=lax.Precision.HIGHEST)
    return rounded(jax.nn.relu(product))


def reference(frames, counts, slot_ids, reset_flags, hidden_state, cell_state, conv_first, conv_second, conv_third, res_first, res_second, projection, input_weight, recur_weight, gate_bias, head_weight):
    hidden_width = hidden_state.shape[0]
    slot_count = hidden_state.shape[1] // N_DP
    starts = jnp.cumsum(counts, axis=1, dtype=jnp.int32) - counts
    range_ends = starts + counts
    tensor_rows = jnp.arange(N_TENSOR, dtype=jnp.int32)
    positions = jnp.arange(ROWS_DEV, dtype=jnp.int32)
    input_rows = input_weight.astype(jnp.float32).reshape(4 * hidden_width, -1)
    recur_rows = recur_weight.astype(jnp.float32).reshape(4 * hidden_width, hidden_width)
    head_rows = head_weight.astype(jnp.float32)
    gate_offset = gate_bias.reshape(4 * hidden_width, 1)

    def one_group(dp_index):
        balanced_ranks = positions[None, :] * N_DP + dp_index
        source = jnp.sum((range_ends[:, :, None] <= balanced_ranks[:, None, :]).astype(jnp.int32), axis=1)
        offset = balanced_ranks - jnp.take_along_axis(starts, source, axis=1)
        arrival = ((source * N_TENSOR + tensor_rows[:, None]) * CAP + offset).reshape(-1).astype(jnp.int32)
        images = jnp.take(frames, arrival, axis=0)
        features = encode(images, conv_first, conv_second, conv_third, res_first, res_second, projection)
        chosen = lax.dynamic_index_in_dim(slot_ids, dp_index, 0, keepdims=False)
        flags = lax.dynamic_index_in_dim(reset_flags, dp_index, 0, keepdims=False)
        keep_state = (1 - jnp.take(flags, chosen)).astype(jnp.float32)
        hidden_group = lax.dynamic_slice_in_dim(hidden_state, dp_index * slot_count, slot_count, 1)
        cell_group = lax.dynamic_slice_in_dim(cell_state, dp_index * slot_count, slot_count, 1)
        prev_hidden = jnp.take(hidden_group, chosen, axis=1) * keep_state[None, :]
        prev_cell = jnp.take(cell_group, chosen, axis=1) * keep_state[None, :]
        gate_sums = jnp.dot(input_rows, features, precision=lax.Precision.HIGHEST)
        gate_sums = gate_sums + jnp.dot(recur_rows, rounded(prev_hidden), precision=lax.Precision.HIGHEST)
        gate_sums = (gate_sums + gate_offset).reshape(4, hidden_width, -1)
        next_cell = jax.nn.sigmoid(gate_sums[1]) * prev_cell + jax.nn.sigmoid(gate_sums[0]) * jnp.tanh(gate_sums[2])
        next_hidden = jax.nn.sigmoid(gate_sums[3]) * jnp.tanh(next_cell)
        head_values = jnp.dot(head_rows, rounded(next_hidden), precision=lax.Precision.HIGHEST)
        return head_values, hidden_group.at[:, chosen].set(next_hidden), cell_group.at[:, chosen].set(next_cell), arrival

    head_values, hidden_groups, cell_groups, arrivals = lax.map(one_group, jnp.arange(N_DP, dtype=jnp.int32))
    outputs_wide = head_values.shape[1]
    policy_out = jnp.zeros((outputs_wide, frames.shape[0]), jnp.float32)
    policy_out = policy_out.at[:, arrivals.reshape(-1)].set(jnp.moveaxis(head_values, 0, 1).reshape(outputs_wide, -1))
    hidden_after = jnp.moveaxis(hidden_groups, 0, 1).reshape(hidden_width, -1)
    cell_after = jnp.moveaxis(cell_groups, 0, 1).reshape(hidden_width, -1)
    return policy_out, hidden_after, cell_after
```

```python
import jax
import jax.numpy as jnp
from jax import lax
from jax.experimental import pallas as pl
from jax.experimental.pallas import tpu as pltpu
from jax.sharding import PartitionSpec as P

BF = jnp.bfloat16
F32 = jnp.float32
NEG = -3.0e38


def lanes(shape, dim):
    return lax.broadcasted_iota(jnp.int32, shape, dim)


def dot(a, b):
    return jnp.dot(a, b, preferred_element_type=F32)


def spread(w, width):
    pick = (lanes((width, 128), 1) % width == lanes((width, 128), 0)).astype(BF)
    return dot(w, pick)


def band_weights(out_ref, tiled, depth, spots, per_lane, columns, first):
    width = 128 // per_lane
    lane = lanes((depth, 128), 1) // width
    for ky in range(3):
        for p in range(spots):
            for col in range(columns):
                block = None
                for i in range(per_lane):
                    start = first(col, i)
                    if start is None:
                        continue
                    kx = p - start
                    if 0 <= kx <= 2:
                        row = (ky * 3 + kx) * depth
                        part = jnp.where(lane == i, tiled[row : row + depth], 0.0)
                        block = part if block is None else block + part
                if block is None:
                    block = jnp.zeros((depth, 128), F32)
                row = (ky * spots + p) * depth
                out_ref[row : row + depth, col * 128 : col * 128 + 128] = block.astype(BF)


def shifted(parts, pitch):
    lane = lanes(parts[0].shape, 1)
    rolled = [pltpu.roll(a, 128 - pitch, 1) for a in parts]
    return [
        jnp.where(lane < 128 - pitch, rolled[v], rolled[min(v + 1, len(parts) - 1)])
        for v in range(len(parts))
    ]


def encoder(
    frames, w1, w2, w3, r1, r2, pt, out,
    raw, flat, sel, k1, k2, k3, kr1, kr2, ptf, ptk, u, carry, p1, p2, p3, p3r, q1, sems,
):
    n = frames.shape[0]
    pairs = frames.shape[1]

    def fetch(q):
        return pltpu.make_async_copy(frames.at[:, q], raw.at[q], sems.at[q])

    def start(q, _):
        fetch(q).start()
        return 0

    lax.fori_loop(0, pairs, start, 0)

    x = lanes((128, 768), 0)
    col = lanes((128, 768), 1)
    p = col % 32
    hit = (x == (col // 128) * 16 - 11 + p) & (p < 18)
    for c in range(4):
        sel[c * 128 : c * 128 + 128] = jnp.where(hit & (col // 32 % 4 == c), 1.0, 0.0).astype(BF)
    t1 = spread(w1[...], 16)
    t1 = jnp.concatenate([t1, t1], axis=1)
    kx = lanes((32, 256), 0) - 2 * (lanes((32, 256), 1) // 16 % 8) - lanes((32, 256), 1) // 128
    for ky in range(3):
        for c in range(4):
            block = jnp.zeros((32, 256), F32)
            for k in range(3):
                row = (ky * 3 + k) * 4 + c
                block = jnp.where(kx == k, t1[row : row + 1], block)
            row = ky * 128 + c * 32
            k1[row : row + 32] = block.astype(BF)
    both = lambda col, i: 2 * i + col
    band_weights(k2, spread(w2[...], 32), 16, 16, 4, 2, both)
    band_weights(k3, spread(w3[...], 32), 32, 12, 4, 2, both)
    same = lambda col, i: None if col * 4 + i > 10 else col * 4 + i - 1
    band_weights(kr1, spread(r1[...], 32), 32, 12, 4, 3, same)
    band_weights(kr2, spread(r2[...], 32), 32, 12, 4, 3, same)

    def widen(i, _):
        rows = pl.ds(i * 352, 352)
        block = pt[rows, :].astype(F32)
        ptf[0, rows, :] = block[:, :128]
        ptf[1, rows, :] = block[:, 128:]
        return 0

    lax.fori_loop(0, 11, widen, 0)

    def reorder(y, _):
        for px in range(11):
            rows = pl.ds(y * 384 + px * 32, 32)
            for h in range(2):
                ptk[rows, h * 128 : h * 128 + 128] = ptf[
                    h, pl.ds(y * 11 + px, 32, stride=121), :
                ].astype(BF)
        ptk[pl.ds(y * 384 + 352, 32), :] = jnp.zeros((32, 256), BF)
        return 0

    lax.fori_loop(0, 11, reorder, 0)

    u[0] = jnp.zeros((n, 768), BF)
    u[2 * pairs + 1] = jnp.zeros((n, 768), BF)
    u[2 * pairs + 2] = jnp.zeros((n, 768), BF)
    p1[0] = jnp.zeros((n, 896), BF)
    p1[43] = jnp.zeros((n, 896), BF)
    p1[44] = jnp.zeros((n, 896), BF)
    p2[0] = jnp.zeros((n, 896), BF)
    p2[22] = jnp.zeros((n, 896), BF)
    p2[23] = jnp.zeros((n, 896), BF)
    for ref in (p3r, q1):
        ref[0] = jnp.zeros((n, 384), BF)
        ref[12] = jnp.zeros((n, 384), BF)
    flat[...] = jnp.zeros_like(flat)

    def windows(q, _):
        fetch(q).wait()
        flat[:, 0:84] = raw[q].astype(F32).reshape(n * 8, 84)
        rows = []
        for y in range(2):
            rows.append(
                jnp.concatenate(
                    [flat[pl.ds(y * 4 + c, n, stride=8), :].astype(BF) for c in range(4)], axis=1
                )
            )
        cut = dot(jnp.concatenate(rows, axis=0), sel[...]).astype(BF)
        u[2 * q + 1] = cut[:n]
        u[2 * q + 2] = cut[n:]
        return 0

    lax.fori_loop(0, pairs, windows, 0)

    def conv_row(src, y, count, step, width, weights):
        taps = [src[y + ky] for ky in range(3)]
        lhs = [
            jnp.concatenate([t[:, v * step : v * step + width] for t in taps], axis=1)
            for v in range(count)
        ]
        return lhs

    def pool_stage(src, dst, count, step, width, weights, per, pitch, offset, limit, last):
        carry[0 : count * n] = dot(
            jnp.concatenate(conv_row(src, 0, count, step, width, weights), axis=0), weights[...]
        )
        lane = lanes((n, 128), 1) // pitch

        def body(y, _):
            lhs = conv_row(src, 2 * y + 1, count, step, width, weights) + conv_row(
                src, 2 * y + 2, count, step, width, weights
            )
            acc = dot(jnp.concatenate(lhs, axis=0), weights[...])
            later = acc[count * n :] * jnp.where(y < last, 1.0, 0.0)
            top = jnp.maximum(jnp.maximum(carry[0 : count * n], acc[: count * n]), later)
            carry[0 : count * n] = later
            top = jnp.maximum(top, 0.0)
            even = [top[v * n : v * n + n, :128] for v in range(count)]
            odd = [top[v * n : v * n + n, 128:] for v in range(count)]
            spots = [lane + (v * per - offset) for v in range(count)]
            even[-1] = jnp.where(spots[-1] < limit, even[-1], 0.0)
            nxt = shifted(even, pitch)
            for v in range(count):
                best = jnp.maximum(jnp.maximum(even[v], odd[v]), nxt[v])
                if v == 0 or v == count - 1:
                    best = jnp.where((spots[v] >= 0) & (spots[v] < limit), best, 0.0)
                dst[y + 1, :, v * 128 : v * 128 + 128] = best.astype(BF)
            dst[y + 1, :, count * 128 : count * 128 + 128] = jnp.zeros((n, 128), BF)
            return 0

        lax.fori_loop(0, last + 1, body, 0)

    pool_stage(u, p1, 6, 128, 128, k1, 8, 16, 5, 42, 41)
    pool_stage(p1, p2, 6, 128, 256, k2, 4, 32, 2, 21, 20)

    lane = lanes((n, 128), 1) // 32
    carry[0 : 3 * n] = jnp.full((3 * n, 256), NEG, F32)

    def third(y, _):
        lhs = conv_row(p2, 2 * y, 3, 256, 384, k3) + conv_row(p2, 2 * y + 1, 3, 256, 384, k3)
        acc = dot(jnp.concatenate(lhs, axis=0), k3[...])
        later = jnp.where(y < 10, acc[3 * n :], NEG)
        top = jnp.maximum(jnp.maximum(carry[0 : 3 * n], acc[: 3 * n]), later)
        carry[0 : 3 * n] = later
        even = [top[v * n : v * n + n, :128] for v in range(3)]
        odd = [top[v * n : v * n + n, 128:] for v in range(3)]
        even[0] = jnp.where(lane == 0, NEG, even[0])
        even[2] = jnp.where(lane == 3, NEG, even[2])
        nxt = shifted(even, 32)
        for v in range(3):
            best = jnp.maximum(jnp.maximum(even[v], odd[v]), nxt[v])
            if v == 2:
                best = jnp.where(lane == 3, 0.0, best)
            p3[y, :, v * 128 : v * 128 + 128] = best.astype(BF)
            p3r[y + 1, :, v * 128 : v * 128 + 128] = jnp.maximum(best, 0.0).astype(BF)
        return 0

    lax.fori_loop(0, 11, third, 0)

    def full_rows(src):
        return jnp.concatenate(
            [jnp.concatenate([src[y + ky] for ky in range(3)], axis=1) for y in range(11)], axis=0
        )

    q1[1:12] = jnp.maximum(dot(full_rows(p3r), kr1[...]), 0.0).astype(BF).reshape(11, n, 384)
    final = dot(full_rows(q1), kr2[...]) + p3[...].reshape(11 * n, 384).astype(F32)
    final = jnp.maximum(final, 0.0).astype(BF)
    line = jnp.concatenate([final[y * n : y * n + n] for y in range(11)], axis=1)
    out[...] = jnp.maximum(dot(line, ptk[...]), 0.0).astype(BF)


def encode(frames, conv_first, conv_second, conv_third, res_first, res_second, projection):
    n = frames.shape[0]
    tiles = frames.transpose(0, 2, 1, 3).reshape(n, 42, 8, 84)
    flatw = lambda w: w.transpose(2, 3, 1, 0).reshape(-1, w.shape[0])
    vm = lambda *s: pltpu.VMEM(s, BF)
    vmf = lambda *s: pltpu.VMEM(s, F32)
    return pl.pallas_call(
        encoder,
        out_shape=jax.ShapeDtypeStruct((n, 256), BF),
        in_specs=[pl.BlockSpec(memory_space=pl.ANY)] + [pl.BlockSpec(memory_space=pltpu.VMEM)] * 6,
        out_specs=pl.BlockSpec(memory_space=pltpu.VMEM),
        scratch_shapes=[
            vm(42, n, 8, 84), vmf(n * 8, 128), vm(512, 768), vm(384, 256), vm(768, 256),
            vm(1152, 256), vm(1152, 384), vm(1152, 384), vmf(2, 3872, 128), vm(4224, 256),
            vm(87, n, 768), vmf(6 * n, 256), vm(45, n, 896), vm(24, n, 896),
            vm(11, n, 384), vm(13, n, 384), vm(13, n, 384), pltpu.SemaphoreType.DMA((42,)),
        ],
        compiler_params=pltpu.CompilerParams(vmem_limit_bytes=60 * 1024 * 1024),
    )(tiles, flatw(conv_first), flatw(conv_second), flatw(conv_third), flatw(res_first), flatw(res_second), projection.T)


def joined_along(blocks, dim):
    lengths = list(blocks.shape[1:])
    lengths[dim] *= blocks.shape[0]
    return jnp.moveaxis(blocks, 0, dim).reshape(lengths)


def gather_together(arrays, axis, dims):
    ravelled = jnp.concatenate([a.reshape(-1) for a in arrays])
    lines, at, outs = (lax.all_gather(ravelled, axis), 0, [])
    for a, dim in zip(arrays, dims):
        blocks = lines[:, at : at + a.size].reshape(-1, *a.shape)
        outs.append(joined_along(blocks, dim))
        at += a.size
    return tuple(outs)


def copy_for_each(shard, axis):
    copies = jnp.broadcast_to(shard, (lax.axis_size(axis), *shard.shape))
    return lax.all_to_all(copies, axis, split_axis=0, concat_axis=0, tiled=True)


def over_copies(shard, axis):
    everything = copy_for_each(shard, axis)
    return jnp.sum(everything, axis=0)


def body(
    frames,
    counts,
    slot_ids,
    reset_flags,
    hidden_state,
    cell_state,
    conv_first,
    conv_second,
    conv_third,
    res_first,
    res_second,
    projection,
    input_weight,
    recur_weight,
    gate_bias,
    head_weight,
):
    dp_count = lax.axis_size("dp")
    tensor_count = lax.axis_size("tensor")
    dp_index = lax.axis_index("dp")
    tensor_index = lax.axis_index("tensor")
    capacity = frames.shape[0]
    pair_depth = capacity // dp_count
    per_device = slot_ids.shape[1] // tensor_count
    tallies = lax.dynamic_index_in_dim(counts, tensor_index, 0, keepdims=False)
    starts = jnp.cumsum(tallies, dtype=jnp.int32) - tallies
    range_ends = starts + tallies
    own_start = lax.dynamic_index_in_dim(starts, dp_index, 0, keepdims=False)
    own_count = lax.dynamic_index_in_dim(tallies, dp_index, 0, keepdims=False)
    peer_index = jnp.arange(dp_count, dtype=jnp.int32)
    levels = jnp.arange(pair_depth, dtype=jnp.int32)
    send_rows = ((peer_index[:, None] - own_start) % dp_count + levels[None, :] * dp_count).reshape(
        -1
    )
    send_live = send_rows < own_count
    send_safe = jnp.minimum(send_rows, capacity - 1)
    balanced_ranks = jnp.arange(per_device, dtype=jnp.int32) * dp_count + dp_index
    source = jnp.sum((range_ends[:, None] <= balanced_ranks[None, :]).astype(jnp.int32), axis=0)
    offset = balanced_ranks - jnp.take(starts, source)
    take_slots = source * pair_depth + offset // dp_count
    own = encode(
        frames, conv_first, conv_second, conv_third, res_first, res_second, projection
    )
    outgoing = jnp.where(
        send_live[:, None], jnp.take(own, send_safe, axis=0), jnp.zeros((), jnp.bfloat16)
    )
    incoming = lax.all_to_all(outgoing, "dp", split_axis=0, concat_axis=0, tiled=True)
    features = jnp.take(incoming, take_slots, axis=0).T
    chosen = slot_ids[0]
    keep_state = (1 - jnp.take(reset_flags[0], chosen)).astype(jnp.float32)
    prev_hidden = jnp.take(hidden_state, chosen, axis=1) * keep_state[None, :]
    prev_cell = jnp.take(cell_state, chosen, axis=1) * keep_state[None, :]
    all_features, all_hidden = gather_together(
        (features, prev_hidden.astype(jnp.bfloat16)), "tensor", (1, 0)
    )
    hidden_share = hidden_state.shape[0]
    gate_sums = jnp.dot(
        input_weight.reshape(4 * hidden_share, -1), all_features, preferred_element_type=jnp.float32
    )
    gate_sums = gate_sums + jnp.dot(
        recur_weight.reshape(4 * hidden_share, -1), all_hidden, preferred_element_type=jnp.float32
    )
    gate_sums = (gate_sums + gate_bias.reshape(4 * hidden_share, 1)).reshape(4, hidden_share, -1)
    next_cell = jax.nn.sigmoid(gate_sums[1]) * prev_cell + jax.nn.sigmoid(gate_sums[0]) * jnp.tanh(
        gate_sums[2]
    )
    next_hidden = jax.nn.sigmoid(gate_sums[3]) * jnp.tanh(next_cell)
    hidden_after = hidden_state.at[:, chosen].set(next_hidden)
    cell_after = cell_state.at[:, chosen].set(next_cell)
    partial_heads = jnp.dot(
        head_weight, next_hidden.astype(jnp.bfloat16), preferred_element_type=jnp.float32
    )
    totals = over_copies(partial_heads, "tensor")
    own_heads = lax.dynamic_slice_in_dim(totals, tensor_index * per_device, per_device, 1)
    back_rows = (dp_index - starts[:, None]) % dp_count + levels[None, :] * dp_count
    back_live = (back_rows < tallies[:, None]).reshape(-1)
    back_place = jnp.minimum((starts[:, None] + back_rows) // dp_count, per_device - 1).reshape(-1)
    outgoing_heads = jnp.where(back_live[None, :], jnp.take(own_heads, back_place, axis=1), 0.0)
    returned = lax.all_to_all(outgoing_heads, "dp", split_axis=1, concat_axis=1, tiled=True)
    arrivals = jnp.arange(capacity, dtype=jnp.int32)
    home_slots = (own_start + arrivals) % dp_count * pair_depth + arrivals // dp_count
    policy_out = jnp.where(
        (arrivals < own_count)[None, :], jnp.take(returned, home_slots, axis=1), 0.0
    )
    return (policy_out, hidden_after, cell_after)


def solution(mesh):
    return jax.shard_map(
        body,
        mesh=mesh,
        in_specs=(
            P(("dp", "tensor"), None, None, None),
            P(),
            P("dp", None),
            P("dp", None),
            P("tensor", "dp"),
            P("tensor", "dp"),
            P(),
            P(),
            P(),
            P(),
            P(),
            P(),
            P(None, "tensor", None),
            P(None, "tensor", None),
            P(None, "tensor"),
            P(None, "tensor"),
        ),
        out_specs=(P(None, ("dp", "tensor")), P("tensor", "dp"), P("tensor", "dp")),
        check_vma=False,
    )
```

```python
import jax
import jax.numpy as jnp
from jax import lax
from jax.experimental import pallas as pl
from jax.experimental.pallas import tpu as pltpu
from jax.sharding import PartitionSpec as P

BF = jnp.bfloat16
F32 = jnp.float32
NEG = -3.0e38


def lanes(shape, dim):
    return lax.broadcasted_iota(jnp.int32, shape, dim)


def dot(a, b):
    return jnp.dot(a, b, preferred_element_type=F32)


def spread(w, width):
    pick = (lanes((width, 128), 1) % width == lanes((width, 128), 0)).astype(BF)
    return dot(w, pick)


def band_weights(out_ref, tiled, depth, spots, per_lane, columns, first):
    width = 128 // per_lane
    lane = lanes((depth, 128), 1) // width
    for ky in range(3):
        for p in range(spots):
            for col in range(columns):
                block = None
                for i in range(per_lane):
                    start = first(col, i)
                    if start is None:
                        continue
                    kx = p - start
                    if 0 <= kx <= 2:
                        row = (ky * 3 + kx) * depth
                        part = jnp.where(lane == i, tiled[row : row + depth], 0.0)
                        block = part if block is None else block + part
                if block is None:
                    block = jnp.zeros((depth, 128), F32)
                row = (ky * spots + p) * depth
                out_ref[row : row + depth, col * 128 : col * 128 + 128] = block.astype(BF)


def shifted(parts, pitch):
    lane = lanes(parts[0].shape, 1)
    rolled = [pltpu.roll(a, 128 - pitch, 1) for a in parts]
    return [
        jnp.where(lane < 128 - pitch, rolled[v], rolled[min(v + 1, len(parts) - 1)])
        for v in range(len(parts))
    ]


def count_tables(counts, me_t, me_d, cap, per):
    nd = counts.shape[1]
    own = counts[pl.ds(me_t, 1), :].astype(F32)
    a_row = lanes((nd, nd), 1)
    a_col = lanes((nd, nd), 0)
    wide = jnp.broadcast_to(own, (nd, nd))
    start_col = jnp.sum(jnp.where(a_row < a_col, wide, 0.0), axis=1, keepdims=True)
    count_col = jnp.sum(jnp.where(a_row == a_col, wide, 0.0), axis=1, keepdims=True)
    start_row = jnp.sum(
        jnp.where(a_col < a_row, jnp.broadcast_to(count_col, (nd, nd)), 0.0), axis=0, keepdims=True
    )
    mine = lanes((1, nd), 1) == me_d
    start = jnp.sum(jnp.where(mine, start_row, 0.0), axis=1, keepdims=True).astype(jnp.int32)
    count = jnp.sum(jnp.where(mine, own, 0.0), axis=1, keepdims=True).astype(jnp.int32)
    b, j = lanes((nd, cap), 0), lanes((nd, cap), 1)
    send = (jnp.bitwise_and(b - start - j, nd - 1) == 0) & (j < count)
    rank = (lanes((per, nd), 0) * nd + me_d).astype(F32)
    take = (start_row <= rank) & (rank < start_row + own)
    rank = (lanes((nd, per), 1) * nd + me_d).astype(F32)
    give = (start_col <= rank) & (rank < start_col + count_col)
    j, b = lanes((cap, nd), 0), lanes((cap, nd), 1)
    home = (jnp.bitwise_and(b - start - j, nd - 1) == 0) & (j < count)
    as_f32 = lambda m: jnp.where(m, 1.0, 0.0)
    return as_f32(send), as_f32(take), as_f32(give), as_f32(home)


def dot_nt(a, b):
    return lax.dot_general(a, b, (((1,), (1,)), ((), ())), preferred_element_type=F32)


def exact(a, b):
    return jnp.dot(a, b, precision=lax.Precision.HIGHEST, preferred_element_type=F32)


class Ring:
    def __init__(self, axis, other):
        self.axis, self.size, self.me = axis, lax.axis_size(axis), lax.axis_index(axis)
        self.other = lax.axis_index(other)

    def place(self, peer):
        return (peer, self.other) if self.axis == "dp" else (self.other, peer)

    def each(self, act):
        def step(k, _):
            act(k, lax.rem(self.me + k, self.size))
            return 0

        lax.fori_loop(1, self.size, step, 0)

    def copy(self, k, peer, src, dst, sems):
        return pltpu.make_async_remote_copy(
            src_ref=src, dst_ref=dst, send_sem=sems.at[0, k], recv_sem=sems.at[1, k],
            device_id=self.place(peer), device_id_type=pl.DeviceIdType.MESH,
        )


def greet(rings):
    barrier = pltpu.get_barrier_semaphore()
    for ring in rings:
        ring.each(
            lambda k, peer, ring=ring: pl.semaphore_signal(
                barrier, inc=1, device_id=ring.place(peer), device_id_type=pl.DeviceIdType.MESH
            )
        )
    pl.semaphore_wait(barrier, sum(ring.size - 1 for ring in rings))


def send_hidden(ring, ids, reset, hid, hall, sems):
    slots, rows = hid.shape[1], ids.shape[1]
    keep = (1 - reset[...]).astype(F32)
    pick = jnp.where(lanes((slots, rows), 0) == ids[...], 1.0, 0.0)
    hall[ring.me] = dot((hid[...] * keep).astype(BF), pick.astype(BF)).astype(BF)
    copy = lambda k, peer: ring.copy(k, peer, hall.at[ring.me], hall.at[ring.me], sems)
    ring.each(lambda k, peer: copy(k, peer).start())
    return copy


def core(
    feat, dp, tp, hidden_copy, waits,
    counts, ids, reset, bias, head, hid, cell, win, wrec,
    out, hout, cout,
    hall, orow, inrow, fall, hp, hin, brow, rrow, gates, sem_f, sem_g, sem_h, sem_b,
):
    cap, per = feat.shape[0], fall.shape[1]
    share, slots = hid.shape
    rows = ids.shape[1]
    send, take, give, home = count_tables(counts, tp.me, dp.me, cap, per)

    spread_rows = dot(send.astype(BF), feat)
    for b in range(dp.size):
        orow[b] = spread_rows[b : b + 1]
    inrow[dp.me] = orow[dp.me]
    row_copy = lambda k, peer: dp.copy(k, peer, orow.at[peer], inrow.at[dp.me], sem_f)
    dp.each(lambda k, peer: row_copy(k, peer).start())

    waits()
    keep = (1 - reset[...]).astype(F32)
    pick = jnp.where(lanes((slots, rows), 0) == ids[...], 1.0, 0.0)
    tp.each(lambda k, peer: hidden_copy(k, peer).wait())
    everyone = hall[...].reshape(tp.size * share, rows)
    recurrent = []
    for q in range(4):
        tall = jnp.transpose(jnp.broadcast_to(bias[q : q + 1, :], (8, share)))[:, 0:1]
        gates[q * share : (q + 1) * share] = dot(wrec[q * share : (q + 1) * share], everyone) + tall
    prev_cell = exact(cell[...] * keep, pick)

    dp.each(lambda k, peer: row_copy(k, peer).wait())
    gathered = jnp.concatenate([inrow[a] for a in range(dp.size)], axis=0)
    fall[tp.me] = dot(take.astype(BF), gathered.astype(BF)).astype(BF)
    feat_copy = lambda k, peer: tp.copy(k, peer, fall.at[tp.me], fall.at[tp.me], sem_g)
    tp.each(lambda k, peer: feat_copy(k, peer).start())
    tp.each(lambda k, peer: feat_copy(k, peer).wait())

    features = fall[...].reshape(rows, fall.shape[2])
    sums = gates[...] + dot_nt(win[...], features)
    gate = [sums[q * share : (q + 1) * share] for q in range(4)]
    next_cell = jax.nn.sigmoid(gate[1]) * prev_cell + jax.nn.sigmoid(gate[0]) * jnp.tanh(gate[2])
    next_hidden = jax.nn.sigmoid(gate[3]) * jnp.tanh(next_cell)
    partial = jnp.transpose(dot(head[...], next_hidden.astype(BF)))
    width = partial.shape[1]
    for t in range(tp.size):
        hp[t, :, 0:width] = partial[t * per : (t + 1) * per]
    hin[tp.me] = hp[tp.me]
    sum_copy = lambda k, peer: tp.copy(k, peer, hp.at[peer], hin.at[tp.me], sem_h)
    tp.each(lambda k, peer: sum_copy(k, peer).start())

    square = lanes((rows, rows), 0) == lanes((rows, rows), 1)
    column = jnp.sum(jnp.where(square, ids[...], 0).astype(F32), axis=1, keepdims=True)
    lay = jnp.where(lanes((rows, slots), 1).astype(F32) == column, 1.0, 0.0)
    chosen = jnp.sum(lay, axis=0, keepdims=True) > 0.0
    hout[...] = jnp.where(chosen, exact(next_hidden, lay), hid[...])
    cout[...] = jnp.where(chosen, exact(next_cell, lay), cell[...])

    tp.each(lambda k, peer: sum_copy(k, peer).wait())
    total = hin[0]
    for t in range(1, tp.size):
        total = total + hin[t]
    back = exact(give, total)
    for a in range(dp.size):
        brow[a] = back[a : a + 1]
    rrow[dp.me] = brow[dp.me]
    back_copy = lambda k, peer: dp.copy(k, peer, brow.at[peer], rrow.at[dp.me], sem_b)
    dp.each(lambda k, peer: back_copy(k, peer).start())
    dp.each(lambda k, peer: back_copy(k, peer).wait())
    heads = exact(home, jnp.concatenate([rrow[a] for a in range(dp.size)], axis=0))
    out[...] = jnp.transpose(heads)[0 : out.shape[0], :]


def encoder(
    fetch, fetch_dense, after_weights, w1, w2, w3, r1, r2, pt,
    raw, flat, sel, k1, k2, k3, kr1, kr2, ptf, ptk, u, carry, p1, p2, p3, p3r, q1,
):
    pairs, n = raw.shape[0:2]

    x = lanes((128, 768), 0)
    col = lanes((128, 768), 1)
    p = col % 32
    hit = (x == (col // 128) * 16 - 11 + p) & (p < 18)
    for c in range(4):
        sel[c * 128 : c * 128 + 128] = jnp.where(hit & (col // 32 % 4 == c), 1.0, 0.0).astype(BF)
    t1 = spread(w1[...], 16)
    t1 = jnp.concatenate([t1, t1], axis=1)
    kx = lanes((32, 256), 0) - 2 * (lanes((32, 256), 1) // 16 % 8) - lanes((32, 256), 1) // 128
    for ky in range(3):
        for c in range(4):
            block = jnp.zeros((32, 256), F32)
            for k in range(3):
                row = (ky * 3 + k) * 4 + c
                block = jnp.where(kx == k, t1[row : row + 1], block)
            row = ky * 128 + c * 32
            k1[row : row + 32] = block.astype(BF)
    both = lambda col, i: 2 * i + col
    band_weights(k2, spread(w2[...], 32), 16, 16, 4, 2, both)
    band_weights(k3, spread(w3[...], 32), 32, 12, 4, 2, both)
    same = lambda col, i: None if col * 4 + i > 10 else col * 4 + i - 1
    band_weights(kr1, spread(r1[...], 32), 32, 12, 4, 3, same)
    band_weights(kr2, spread(r2[...], 32), 32, 12, 4, 3, same)

    after_weights()
    fetch_dense()

    def widen(i, _):
        rows = pl.ds(i * 352, 352)
        block = pt[rows, :].astype(F32)
        ptf[0, rows, :] = block[:, :128]
        ptf[1, rows, :] = block[:, 128:]
        return 0

    lax.fori_loop(0, 11, widen, 0)

    def reorder(y, _):
        for px in range(11):
            rows = pl.ds(y * 384 + px * 32, 32)
            for h in range(2):
                ptk[rows, h * 128 : h * 128 + 128] = ptf[
                    h, pl.ds(y * 11 + px, 32, stride=121), :
                ].astype(BF)
        ptk[pl.ds(y * 384 + 352, 32), :] = jnp.zeros((32, 256), BF)
        return 0

    lax.fori_loop(0, 11, reorder, 0)

    u[0] = jnp.zeros((n, 768), BF)
    u[2 * pairs + 1] = jnp.zeros((n, 768), BF)
    u[2 * pairs + 2] = jnp.zeros((n, 768), BF)
    p1[0] = jnp.zeros((n, 896), BF)
    p1[43] = jnp.zeros((n, 896), BF)
    p1[44] = jnp.zeros((n, 896), BF)
    p2[0] = jnp.zeros((n, 896), BF)
    p2[22] = jnp.zeros((n, 896), BF)
    p2[23] = jnp.zeros((n, 896), BF)
    for ref in (p3r, q1):
        ref[0] = jnp.zeros((n, 384), BF)
        ref[12] = jnp.zeros((n, 384), BF)
    flat[...] = jnp.zeros_like(flat)

    def windows(q, _):
        fetch(q).wait()
        flat[:, 0:84] = raw[q].astype(F32).reshape(n * 8, 84)
        rows = []
        for y in range(2):
            rows.append(
                jnp.concatenate(
                    [flat[pl.ds(y * 4 + c, n, stride=8), :].astype(BF) for c in range(4)], axis=1
                )
            )
        cut = dot(jnp.concatenate(rows, axis=0), sel[...]).astype(BF)
        u[2 * q + 1] = cut[:n]
        u[2 * q + 2] = cut[n:]
        return 0

    lax.fori_loop(0, pairs, windows, 0)

    def conv_row(src, y, count, step, width, weights):
        taps = [src[y + ky] for ky in range(3)]
        lhs = [
            jnp.concatenate([t[:, v * step : v * step + width] for t in taps], axis=1)
            for v in range(count)
        ]
        return lhs

    def pool_stage(src, dst, count, step, width, weights, per, pitch, offset, limit, last):
        carry[0 : count * n] = dot(
            jnp.concatenate(conv_row(src, 0, count, step, width, weights), axis=0), weights[...]
        )
        lane = lanes((n, 128), 1) // pitch

        def body(y, _):
            lhs = conv_row(src, 2 * y + 1, count, step, width, weights) + conv_row(
                src, 2 * y + 2, count, step, width, weights
            )
            acc = dot(jnp.concatenate(lhs, axis=0), weights[...])
            later = acc[count * n :] * jnp.where(y < last, 1.0, 0.0)
            top = jnp.maximum(jnp.maximum(carry[0 : count * n], acc[: count * n]), later)
            carry[0 : count * n] = later
            top = jnp.maximum(top, 0.0)
            even = [top[v * n : v * n + n, :128] for v in range(count)]
            odd = [top[v * n : v * n + n, 128:] for v in range(count)]
            spots = [lane + (v * per - offset) for v in range(count)]
            even[-1] = jnp.where(spots[-1] < limit, even[-1], 0.0)
            nxt = shifted(even, pitch)
            for v in range(count):
                best = jnp.maximum(jnp.maximum(even[v], odd[v]), nxt[v])
                if v == 0 or v == count - 1:
                    best = jnp.where((spots[v] >= 0) & (spots[v] < limit), best, 0.0)
                dst[y + 1, :, v * 128 : v * 128 + 128] = best.astype(BF)
            dst[y + 1, :, count * 128 : count * 128 + 128] = jnp.zeros((n, 128), BF)
            return 0

        lax.fori_loop(0, last + 1, body, 0)

    pool_stage(u, p1, 6, 128, 128, k1, 8, 16, 5, 42, 41)
    pool_stage(p1, p2, 6, 128, 256, k2, 4, 32, 2, 21, 20)

    lane = lanes((n, 128), 1) // 32
    carry[0 : 3 * n] = jnp.full((3 * n, 256), NEG, F32)

    def third(y, _):
        lhs = conv_row(p2, 2 * y, 3, 256, 384, k3) + conv_row(p2, 2 * y + 1, 3, 256, 384, k3)
        acc = dot(jnp.concatenate(lhs, axis=0), k3[...])
        later = jnp.where(y < 10, acc[3 * n :], NEG)
        top = jnp.maximum(jnp.maximum(carry[0 : 3 * n], acc[: 3 * n]), later)
        carry[0 : 3 * n] = later
        even = [top[v * n : v * n + n, :128] for v in range(3)]
        odd = [top[v * n : v * n + n, 128:] for v in range(3)]
        even[0] = jnp.where(lane == 0, NEG, even[0])
        even[2] = jnp.where(lane == 3, NEG, even[2])
        nxt = shifted(even, 32)
        for v in range(3):
            best = jnp.maximum(jnp.maximum(even[v], odd[v]), nxt[v])
            if v == 2:
                best = jnp.where(lane == 3, 0.0, best)
            p3[y, :, v * 128 : v * 128 + 128] = best.astype(BF)
            p3r[y + 1, :, v * 128 : v * 128 + 128] = jnp.maximum(best, 0.0).astype(BF)
        return 0

    lax.fori_loop(0, 11, third, 0)

    def full_rows(src):
        return jnp.concatenate(
            [jnp.concatenate([src[y + ky] for ky in range(3)], axis=1) for y in range(11)], axis=0
        )

    q1[1:12] = jnp.maximum(dot(full_rows(p3r), kr1[...]), 0.0).astype(BF).reshape(11, n, 384)
    final = dot(full_rows(q1), kr2[...]) + p3[...].reshape(11 * n, 384).astype(F32)
    final = jnp.maximum(final, 0.0).astype(BF)
    line = jnp.concatenate([final[y * n : y * n + n] for y in range(11)], axis=1)
    return jnp.maximum(dot(line, ptk[...]), 0.0).astype(BF)


def step(
    frames, proj, hidden, cells, w_in, w_rec, w1, w2, w3, r1, r2, counts, ids, reset, bias, head,
    out, hout, cout, *scratch,
):
    raw, enc, (pt, hid, cell, win, wrec, hall), own = scratch[0], scratch[1:17], scratch[17:23], scratch[23:35]
    sem_q, sem_w, sem_x = scratch[35:]
    dp, tp = Ring("dp", "tensor"), Ring("tensor", "dp")
    pairs = raw.shape[0]
    loads = [
        pltpu.make_async_copy(src, dst, sem_w.at[i])
        for i, (src, dst) in enumerate(
            [(hidden, hid), (proj, pt), (w_rec, wrec), (w_in, win), (cells, cell)]
        )
    ]

    def fetch(q):
        return pltpu.make_async_copy(frames.at[:, q], raw.at[q], sem_q.at[q])

    def start(q, _):
        fetch(q).start()
        return 0

    loads[0].start()
    loads[1].start()
    lax.fori_loop(0, pairs, start, 0)
    for load in loads[2:]:
        load.start()
    own[4][...] = jnp.zeros_like(own[4])
    sent = []

    def share_hidden():
        loads[0].wait()
        greet((dp, tp))
        sent.append(send_hidden(tp, ids, reset, hid, hall, sem_x))

    def rest():
        for load in loads[2:]:
            load.wait()

    feat = encoder(fetch, loads[1].wait, share_hidden, w1, w2, w3, r1, r2, pt, raw, *enc)
    core(
        feat, dp, tp, sent[0], rest, counts, ids, reset, bias, head, hid, cell, win, wrec,
        out, hout, cout, hall, *own,
    )


def body(
    frames, counts, slot_ids, reset_flags, hidden_state, cell_state, conv_first, conv_second,
    conv_third, res_first, res_second, projection, input_weight, recur_weight, gate_bias, head_weight,
):
    n = frames.shape[0]
    share, slots = hidden_state.shape
    nd, nt = lax.axis_size("dp"), lax.axis_size("tensor")
    rows = slot_ids.shape[1]
    per = rows // nt
    tiles = frames.transpose(0, 2, 1, 3).reshape(n, 42, 8, 84)
    flatw = lambda w: w.transpose(2, 3, 1, 0).reshape(-1, w.shape[0])
    vm = lambda *s: pltpu.VMEM(s, BF)
    vmf = lambda *s: pltpu.VMEM(s, F32)
    pairs = lambda m: pltpu.SemaphoreType.DMA((2, m))
    anywhere = pl.BlockSpec(memory_space=pl.ANY)
    local = pl.BlockSpec(memory_space=pltpu.VMEM)
    width = input_weight.shape[2]
    return pl.pallas_call(
        step,
        out_shape=[
            jax.ShapeDtypeStruct((head_weight.shape[0], n), F32),
            jax.ShapeDtypeStruct((share, slots), F32),
            jax.ShapeDtypeStruct((share, slots), F32),
        ],
        in_specs=[anywhere] * 6 + [local] * 10,
        out_specs=[local] * 3,
        scratch_shapes=[
            vm(42, n, 8, 84),
            vmf(n * 8, 128), vm(512, 768), vm(384, 256), vm(768, 256),
            vm(1152, 256), vm(1152, 384), vm(1152, 384), vmf(2, 3872, 128), vm(4224, 256),
            vm(87, n, 768), vmf(6 * n, 256), vm(45, n, 896), vm(24, n, 896),
            vm(11, n, 384), vm(13, n, 384), vm(13, n, 384),
            vm(3872, 256), vmf(share, slots), vmf(share, slots), vm(4 * share, width),
            vm(4 * share, nt * share), vm(nt, share, rows),
            vmf(nd, 1, width), vmf(nd, 1, width), vm(nt, per, width), vmf(nt, per, 128),
            vmf(nt, per, 128), vmf(nd, 1, 128), vmf(nd, 1, 128), vmf(4 * share, rows),
            pairs(nd), pairs(nt), pairs(nt), pairs(nd),
            pltpu.SemaphoreType.DMA((42,)), pltpu.SemaphoreType.DMA((5,)), pairs(nt),
        ],
        compiler_params=pltpu.CompilerParams(
            vmem_limit_bytes=60 * 1024 * 1024, collective_id=0, has_side_effects=True
        ),
    )(
        tiles, projection.T, hidden_state, cell_state, input_weight.reshape(4 * share, width),
        recur_weight.reshape(4 * share, nt * share), flatw(conv_first), flatw(conv_second),
        flatw(conv_third), flatw(res_first), flatw(res_second), counts, slot_ids, reset_flags,
        gate_bias, jnp.pad(head_weight, ((0, 13), (0, 0))),
    )


def solution(mesh):
    return jax.shard_map(
        body,
        mesh=mesh,
        in_specs=(
            P(("dp", "tensor"), None, None, None),
            P(),
            P("dp", None),
            P("dp", None),
            P("tensor", "dp"),
            P("tensor", "dp"),
            P(),
            P(),
            P(),
            P(),
            P(),
            P(),
            P(None, "tensor", None),
            P(None, "tensor", None),
            P(None, "tensor"),
            P(None, "tensor"),
        ),
        out_specs=(P(None, ("dp", "tensor")), P("tensor", "dp"), P("tensor", "dp")),
        check_vma=False,
    )
```

```python
import jax
import jax.numpy as jnp
from jax import lax
from jax.experimental import pallas as pl
from jax.experimental.pallas import tpu as pltpu
from jax.sharding import PartitionSpec as P

BF = jnp.bfloat16
F32 = jnp.float32
NEG = -3.0e38


def lanes(shape, dim):
    return lax.broadcasted_iota(jnp.int32, shape, dim)


def dot(a, b):
    return jnp.dot(a, b, preferred_element_type=F32)


def spread(w, width):
    pick = (lanes((width, 128), 1) % width == lanes((width, 128), 0)).astype(BF)
    return dot(w, pick)


def spread_turned(w):
    pick = (lanes((32, 128), 1) % 32 == lanes((32, 128), 0)).astype(BF)
    return jnp.concatenate(
        [
            lax.dot_general(
                w[k * 32 : k * 32 + 32, :], pick, (((0,), (0,)), ((), ())), preferred_element_type=F32
            )
            for k in range(9)
        ],
        axis=0,
    )


def band_weights(out_ref, tiled, depth, spots, per_lane, columns, first):
    width = 128 // per_lane
    lane = lanes((depth, 128), 1) // width
    for ky in range(3):
        for p in range(spots):
            for col in range(columns):
                block = None
                for i in range(per_lane):
                    start = first(col, i)
                    if start is None:
                        continue
                    kx = p - start
                    if 0 <= kx <= 2:
                        row = (ky * 3 + kx) * depth
                        part = jnp.where(lane == i, tiled[row : row + depth], 0.0)
                        block = part if block is None else block + part
                if block is None:
                    block = jnp.zeros((depth, 128), F32)
                row = (ky * spots + p) * depth
                out_ref[row : row + depth, col * 128 : col * 128 + 128] = block.astype(BF)


def column_mask(n, test):
    return jnp.where(test(lanes((n, 128), 1)), 1.0, 0.0).astype(BF)


def shifted(parts, pitch):
    inside = column_mask(parts[0].shape[0], lambda lane: lane < 128 - pitch) > 0.5
    rolled = [pltpu.roll(a, 128 - pitch, 1) for a in parts]
    return [
        jnp.where(inside, rolled[v], rolled[min(v + 1, len(parts) - 1)])
        for v in range(len(parts))
    ]


def alternate(count, produce, consume):
    produce(0, 0)

    def body(i, _):
        produce(2 * i + 1, 1)
        consume(2 * i, 0)
        produce(2 * i + 2, 0)
        consume(2 * i + 1, 1)
        return 0

    lax.fori_loop(0, (count - 1) // 2, body, 0)
    consume(count - 1, 0)


def count_tables(counts, me_t, me_d, cap, per):
    nd = counts.shape[1]
    own = counts[pl.ds(me_t, 1), :].astype(F32)
    a_row = lanes((nd, nd), 1)
    a_col = lanes((nd, nd), 0)
    wide = jnp.broadcast_to(own, (nd, nd))
    start_col = jnp.sum(jnp.where(a_row < a_col, wide, 0.0), axis=1, keepdims=True)
    count_col = jnp.sum(jnp.where(a_row == a_col, wide, 0.0), axis=1, keepdims=True)
    start_row = jnp.sum(
        jnp.where(a_col < a_row, jnp.broadcast_to(count_col, (nd, nd)), 0.0), axis=0, keepdims=True
    )
    mine = lanes((1, nd), 1) == me_d
    start = jnp.sum(jnp.where(mine, start_row, 0.0), axis=1, keepdims=True).astype(jnp.int32)
    count = jnp.sum(jnp.where(mine, own, 0.0), axis=1, keepdims=True).astype(jnp.int32)
    b, j = lanes((nd, cap), 0), lanes((nd, cap), 1)
    send = (jnp.bitwise_and(b - start - j, nd - 1) == 0) & (j < count)
    rank = (lanes((per, nd), 0) * nd + me_d).astype(F32)
    take = (start_row <= rank) & (rank < start_row + own)
    rank = (lanes((nd, per), 1) * nd + me_d).astype(F32)
    give = (start_col <= rank) & (rank < start_col + count_col)
    j, b = lanes((cap, nd), 0), lanes((cap, nd), 1)
    home = (jnp.bitwise_and(b - start - j, nd - 1) == 0) & (j < count)
    as_f32 = lambda m: jnp.where(m, 1.0, 0.0)
    return as_f32(send), as_f32(take), as_f32(give), as_f32(home)


def dot_nt(a, b):
    return lax.dot_general(a, b, (((1,), (1,)), ((), ())), preferred_element_type=F32)


def chosen_rows(a, b, turn=False):
    value, pick = (a, b.astype(BF)) if turn else (b, a.astype(BF))
    high = value.astype(BF)
    rest = value - high.astype(F32)
    middle = rest.astype(BF)
    terms = (high, middle, (rest - middle.astype(F32)).astype(BF))
    parts = [dot(t, pick) if turn else dot(pick, t) for t in terms]
    return parts[0] + parts[1] + parts[2]


class Ring:
    def __init__(self, axis, other):
        self.axis, self.size, self.me = axis, lax.axis_size(axis), lax.axis_index(axis)
        self.other = lax.axis_index(other)

    def place(self, peer):
        return (peer, self.other) if self.axis == "dp" else (self.other, peer)

    def each(self, act):
        def step(i, _):
            k = 1 + lax.rem(i + self.size * 3 // 8, self.size - 1)
            act(k, lax.rem(self.me + k, self.size))
            return 0

        lax.fori_loop(0, self.size - 1, step, 0)

    def copy(self, k, peer, src, dst, sems):
        return pltpu.make_async_remote_copy(
            src_ref=src, dst_ref=dst, send_sem=sems.at[0, k], recv_sem=sems.at[1, k],
            device_id=self.place(peer), device_id_type=pl.DeviceIdType.MESH,
        )


def greet(rings):
    barrier = pltpu.get_barrier_semaphore()
    for ring in rings:
        ring.each(
            lambda k, peer, ring=ring: pl.semaphore_signal(
                barrier, inc=1, device_id=ring.place(peer), device_id_type=pl.DeviceIdType.MESH
            )
        )
    pl.semaphore_wait(barrier, sum(ring.size - 1 for ring in rings))


def send_hidden(ring, ids, reset, hid, hall, sems):
    slots, rows = hid.shape[1], ids.shape[1]
    keep = (1 - reset[...]).astype(F32)
    pick = jnp.where(lanes((slots, rows), 0) == ids[...], 1.0, 0.0)
    hall[ring.me] = dot((hid[...] * keep).astype(BF), pick.astype(BF)).astype(BF)
    copy = lambda k, peer: ring.copy(k, peer, hall.at[ring.me], hall.at[ring.me], sems)
    ring.each(lambda k, peer: copy(k, peer).start())
    return copy


def core(
    feat, dp, tp, hidden_copy, waits, tables, stores,
    ids, reset, bias, head, hid, cell, win, wrec,
    out, hout, cout,
    hall, orow, inrow, fall, hp, hin, brow, rrow, gates, sem_f, sem_g, sem_h, sem_b,
):
    per = fall.shape[1]
    share, slots = hid.shape
    rows = ids.shape[1]
    send, take, give, home = tables

    spread_rows = dot(send.astype(BF), feat)
    for b in range(dp.size):
        orow[b] = spread_rows[b : b + 1]
    inrow[dp.me] = orow[dp.me]
    row_copy = lambda k, peer: dp.copy(k, peer, orow.at[peer], inrow.at[dp.me], sem_f)
    dp.each(lambda k, peer: row_copy(k, peer).start())

    waits()
    keep = (1 - reset[...]).astype(F32)
    pick = jnp.where(lanes((slots, rows), 0) == ids[...], 1.0, 0.0)
    tp.each(lambda k, peer: hidden_copy(k, peer).wait())
    everyone = hall[...].reshape(tp.size * share, rows)
    recurrent = []
    for q in range(4):
        tall = jnp.transpose(jnp.broadcast_to(bias[q : q + 1, :], (8, share)))[:, 0:1]
        gates[q * share : (q + 1) * share] = dot(wrec[q * share : (q + 1) * share], everyone) + tall
    prev_cell = chosen_rows(cell[...] * keep, pick, True)

    dp.each(lambda k, peer: row_copy(k, peer).wait())
    gathered = jnp.concatenate([inrow[a] for a in range(dp.size)], axis=0)
    fall[tp.me] = dot(take.astype(BF), gathered.astype(BF)).astype(BF)
    feat_copy = lambda k, peer: tp.copy(k, peer, fall.at[tp.me], fall.at[tp.me], sem_g)
    tp.each(lambda k, peer: feat_copy(k, peer).start())
    tp.each(lambda k, peer: feat_copy(k, peer).wait())

    features = fall[...].reshape(rows, fall.shape[2])
    sums = gates[...] + dot_nt(win[...], features)
    gate = [sums[q * share : (q + 1) * share] for q in range(4)]
    next_cell = jax.nn.sigmoid(gate[1]) * prev_cell + jax.nn.sigmoid(gate[0]) * jnp.tanh(gate[2])
    next_hidden = jax.nn.sigmoid(gate[3]) * jnp.tanh(next_cell)
    partial = jnp.transpose(dot(head[...], next_hidden.astype(BF)))
    width = partial.shape[1]
    for t in range(tp.size):
        hp[t, :, 0:width] = partial[t * per : (t + 1) * per]
    hin[tp.me] = hp[tp.me]
    sum_copy = lambda k, peer: tp.copy(k, peer, hp.at[peer], hin.at[tp.me], sem_h)
    tp.each(lambda k, peer: sum_copy(k, peer).start())

    square = lanes((rows, rows), 0) == lanes((rows, rows), 1)
    column = jnp.sum(jnp.where(square, ids[...], 0).astype(F32), axis=1, keepdims=True)
    lay = jnp.where(lanes((rows, slots), 1).astype(F32) == column, 1.0, 0.0)
    chosen = jnp.sum(lay, axis=0, keepdims=True) > 0.0
    hout[...] = jnp.where(chosen, chosen_rows(next_hidden, lay, True), hid[...])
    cout[...] = jnp.where(chosen, chosen_rows(next_cell, lay, True), cell[...])

    for store in stores:
        store.start()
    tp.each(lambda k, peer: sum_copy(k, peer).wait())
    total = hin[0]
    for t in range(1, tp.size):
        total = total + hin[t]
    back = chosen_rows(give, total)
    for a in range(dp.size):
        brow[a] = back[a : a + 1]
    rrow[dp.me] = brow[dp.me]
    back_copy = lambda k, peer: dp.copy(k, peer, brow.at[peer], rrow.at[dp.me], sem_b)
    dp.each(lambda k, peer: back_copy(k, peer).start())
    dp.each(lambda k, peer: back_copy(k, peer).wait())
    heads = chosen_rows(home, jnp.concatenate([rrow[a] for a in range(dp.size)], axis=0))
    out[...] = jnp.transpose(heads)[0 : out.shape[0], :]
    for store in stores:
        store.wait()


def encoder(
    fetch, ready, after_weights, w1, w2, w3, r1, r2, pt,
    raw, flat, sel, k1, k2, k3, kr1, kr2, ptf, ptk, u, carry, p1, p2, p3, p3r, q1,
    wide0, wide1, acc0, acc1, third,
):
    pairs, n = raw.shape[0:2]
    wide, acc = (wide0, wide1), (acc0, acc1)
    ready("conv")
    x = lanes((128, 768), 0)
    col = lanes((128, 768), 1)
    p = col % 32
    hit = (x == (col // 128) * 16 - 11 + p) & (p < 18)
    for c in range(4):
        sel[c * 128 : c * 128 + 128] = jnp.where(hit & (col // 32 % 4 == c), 1.0, 0.0).astype(BF)
    t1 = [spread(w1[k // 3, k % 3], 16) for k in range(9)]
    t1 = [jnp.concatenate([t, t], axis=1) for t in t1]
    kx = lanes((32, 256), 0) - 2 * (lanes((32, 256), 1) // 16 % 8) - lanes((32, 256), 1) // 128
    for ky in range(3):
        for c in range(4):
            block = jnp.zeros((32, 256), F32)
            for k in range(3):
                block = jnp.where(kx == k, t1[ky * 3 + k][c : c + 1], block)
            row = ky * 128 + c * 32
            k1[row : row + 32] = block.astype(BF)
    both = lambda col, i: 2 * i + col
    band_weights(k2, spread(w2[...], 32), 16, 16, 4, 2, both)
    band_weights(k3, spread_turned(w3), 32, 12, 4, 2, both)
    same = lambda col, i: None if col * 4 + i > 10 else col * 4 + i - 1
    band_weights(kr1, spread_turned(r1), 32, 12, 4, 3, same)
    band_weights(kr2, spread_turned(r2), 32, 12, 4, 3, same)

    after_weights()
    ready("dense")

    def widen(i, _):
        rows = pl.ds(i * 352, 352)
        block = pt[rows, :].astype(F32)
        ptf[0, rows, :] = block[:, :128]
        ptf[1, rows, :] = block[:, 128:]
        return 0

    lax.fori_loop(0, 11, widen, 0)

    def reorder(y, _):
        for px in range(11):
            rows = pl.ds(y * 384 + px * 32, 32)
            for h in range(2):
                ptk[rows, h * 128 : h * 128 + 128] = ptf[
                    h, pl.ds(y * 11 + px, 32, stride=121), :
                ].astype(BF)
        ptk[pl.ds(y * 384 + 352, 32), :] = jnp.zeros((32, 256), BF)
        return 0

    lax.fori_loop(0, 11, reorder, 0)

    u[0] = jnp.zeros((n, 768), BF)
    u[2 * pairs + 1] = jnp.zeros((n, 768), BF)
    u[2 * pairs + 2] = jnp.zeros((n, 768), BF)
    p1[0] = jnp.zeros((n, 896), BF)
    p1[43] = jnp.zeros((n, 896), BF)
    p1[44] = jnp.zeros((n, 896), BF)
    p2[0] = jnp.zeros((n, 896), BF)
    p2[22] = jnp.zeros((n, 896), BF)
    p2[23] = jnp.zeros((n, 896), BF)
    for ref in (p3r, q1):
        ref[0] = jnp.zeros((n, 384), BF)
        ref[12] = jnp.zeros((n, 384), BF)
    flat[...] = jnp.zeros_like(flat)

    batch = 6

    def unpack(i, slot):
        for g in range(batch):
            q = i * batch + g
            fetch(q).wait()
            flat[slot, g, :, 0:84] = raw[q].astype(F32).reshape(n * 8, 84)
        for g in range(batch):
            for y in range(2):
                for c in range(4):
                    wide[slot][(g * 2 + y) * n : (g * 2 + y + 1) * n, c * 128 : c * 128 + 128] = (
                        flat[slot, g, pl.ds(y * 4 + c, n, stride=8), :].astype(BF)
                    )

    def cut(i, slot):
        got = dot(wide[slot][...], sel[...]).astype(BF)
        u[pl.ds(i * 2 * batch + 1, 2 * batch)] = got.reshape(2 * batch, n, 768)

    alternate(pairs // batch, unpack, cut)

    def conv_row(src, y, count, step, width):
        taps = [src[y + ky] for ky in range(3)]
        return [
            jnp.concatenate([t[:, v * step : v * step + width] for t in taps], axis=1)
            for v in range(count)
        ]

    def conv_rows(src, y, rows, count, step, width, weights):
        lhs = [a for r in range(rows) for a in conv_row(src, y + r, count, step, width)]
        return dot(jnp.concatenate(lhs, axis=0), weights[...]).astype(BF)

    zero = jnp.zeros((), BF)

    def pool_stage(src, dst, group, count, step, width, weights, per, pitch, offset, limit, last):
        size = count * n
        carry[0:size] = conv_rows(src, 0, 1, count, step, width, weights)
        first = column_mask(n, lambda lane: lane // pitch >= offset) > 0.5
        final = column_mask(
            n, lambda lane: lane // pitch + ((count - 1) * per - offset) < limit
        ) > 0.5

        def produce(i, slot):
            acc[slot][0 : 2 * group * size] = conv_rows(
                src, 2 * group * i + 1, 2 * group, count, step, width, weights
            )

        def consume(i, slot):
            for g in range(group):
                y = i * group + g
                row = lambda r, v, h: acc[slot][
                    r * size + v * n : r * size + v * n + n, h * 128 : h * 128 + 128
                ]
                keep = jnp.where(y < last, 1.0, 0.0).astype(BF) if g == group - 1 else None
                half = []
                for h in range(2):
                    tops = []
                    for v in range(count):
                        now, later = row(2 * g, v, h), row(2 * g + 1, v, h)
                        if keep is not None:
                            later = later * keep
                        if g == 0:
                            before = carry[v * n : v * n + n, h * 128 : h * 128 + 128]
                        else:
                            before = row(2 * g - 1, v, h)
                        tops.append(jnp.maximum(jnp.maximum(before, now), jnp.maximum(later, zero)))
                        if g == group - 1:
                            carry[v * n : v * n + n, h * 128 : h * 128 + 128] = later
                    half.append(tops)
                even, odd = half
                even[-1] = jnp.where(final, even[-1], zero)
                nxt = shifted(even, pitch)
                for v in range(count):
                    best = jnp.maximum(jnp.maximum(even[v], odd[v]), nxt[v])
                    if v == 0:
                        best = jnp.where(first, best, zero)
                    if v == count - 1:
                        best = jnp.where(final, best, zero)
                    dst[y + 1, :, v * 128 : v * 128 + 128] = best
                dst[y + 1, :, count * 128 : count * 128 + 128] = jnp.zeros((n, 128), BF)

        alternate((last + 1) // group, produce, consume)

    pool_stage(u, p1, 2, 6, 128, 128, k1, 8, 16, 5, 42, 41)
    pool_stage(p1, p2, 1, 6, 128, 256, k2, 4, 32, 2, 21, 20)

    for y in range(0, 21, 7):
        third[y * 3 * n : (y + 7) * 3 * n] = conv_rows(p2, y, 7, 3, 256, 384, k3)
    low = jnp.full((), NEG, BF)
    begin = column_mask(n, lambda lane: lane >= 32) > 0.5
    inner = column_mask(n, lambda lane: lane < 96) > 0.5
    for y in range(11):
        half = []
        for h in range(2):
            tops = []
            for v in range(3):
                top = None
                for r in range(max(2 * y - 1, 0), min(2 * y + 2, 21)):
                    at = (r * 3 + v) * n
                    part = third[at : at + n, h * 128 : h * 128 + 128]
                    top = part if top is None else jnp.maximum(top, part)
                tops.append(top)
            half.append(tops)
        even, odd = half
        even[0] = jnp.where(begin, even[0], low)
        even[2] = jnp.where(inner, even[2], low)
        nxt = shifted(even, 32)
        for v in range(3):
            best = jnp.maximum(jnp.maximum(even[v], odd[v]), nxt[v])
            if v == 2:
                best = jnp.where(inner, best, zero)
            p3[y, :, v * 128 : v * 128 + 128] = best
            p3r[y + 1, :, v * 128 : v * 128 + 128] = jnp.maximum(best, zero)

    def full_rows(src):
        return jnp.concatenate(
            [jnp.concatenate([src[y + ky] for ky in range(3)], axis=1) for y in range(11)], axis=0
        )

    q1[1:12] = jnp.maximum(dot(full_rows(p3r), kr1[...]), 0.0).astype(BF).reshape(11, n, 384)
    final = dot(full_rows(q1), kr2[...]) + p3[...].reshape(11 * n, 384).astype(F32)
    final = jnp.maximum(final, 0.0).astype(BF)
    line = jnp.concatenate([final[y * n : y * n + n] for y in range(11)], axis=1)
    return jnp.maximum(dot(line, ptk[...]), 0.0).astype(BF)


def step(*refs):
    hbm, (out, hout, cout) = refs[:16], refs[16:19]
    held, (raw, *enc), own = refs[19:34], refs[34:34 + 22], refs[34 + 22:46 + 22]
    hnew, cnew, hall, sem_q, sem_w, sem_x, sem_o = refs[46 + 22:]
    dp, tp = Ring("dp", "tensor"), Ring("tensor", "dp")
    frames = hbm[0]
    loads = [pltpu.make_async_copy(hbm[i + 1], held[i], sem_w.at[i]) for i in range(15)]
    names = ("pt", "hid", "cell", "win", "wrec", "w1", "w2", "w3", "r1", "r2")
    at = {name: i for i, name in enumerate(names + ("counts", "ids", "reset", "bias", "head"))}
    ref = lambda *which: [held[at[name]] for name in which]
    groups = {
        "conv": ("w1", "w2", "w3", "r1", "r2"),
        "dense": ("pt",),
        "hidden": ("hid", "counts", "ids", "reset"),
        "rest": ("cell", "win", "wrec", "bias", "head"),
    }

    def ready(group):
        for name in groups[group]:
            loads[at[name]].wait()

    def fetch(q):
        return pltpu.make_async_copy(frames.at[:, q], raw.at[q], sem_q.at[q])

    def start(q, _):
        fetch(q).start()
        return 0

    for name in groups["conv"] + groups["hidden"]:
        loads[at[name]].start()
    lax.fori_loop(0, raw.shape[0], start, 0)
    for name in groups["dense"] + groups["rest"]:
        loads[at[name]].start()
    own[4][...] = jnp.zeros_like(own[4])
    sent = []
    counts, ids, reset, hid = ref("counts", "ids", "reset", "hid")

    def share_hidden():
        ready("hidden")
        sent.extend(count_tables(counts, tp.me, dp.me, frames.shape[0], own[2].shape[1]))
        greet((dp, tp))
        sent.append(send_hidden(tp, ids, reset, hid, hall, sem_x))

    feat = encoder(fetch, ready, share_hidden, *ref(*groups["conv"], "pt"), raw, *enc)
    stores = [
        pltpu.make_async_copy(hnew, hout, sem_o.at[0]),
        pltpu.make_async_copy(cnew, cout, sem_o.at[1]),
    ]
    core(
        feat, dp, tp, sent[4], lambda: ready("rest"), sent[0:4], stores, ids, reset,
        *ref("bias", "head", "hid", "cell", "win", "wrec"), out, hnew, cnew, hall, *own,
    )


def hand_over(*refs):
    for i in range(3):
        refs[3 + i][...] = refs[i][...]


def body(
    frames, counts, slot_ids, reset_flags, hidden_state, cell_state, conv_first, conv_second,
    conv_third, res_first, res_second, projection, input_weight, recur_weight, gate_bias, head_weight,
):
    n = frames.shape[0]
    share, slots = hidden_state.shape
    nd, nt = lax.axis_size("dp"), lax.axis_size("tensor")
    rows = slot_ids.shape[1]
    per = rows // nt
    width = input_weight.shape[2]
    vm = lambda *s: pltpu.VMEM(s, BF)
    vmf = lambda *s: pltpu.VMEM(s, F32)
    pairs = lambda m: pltpu.SemaphoreType.DMA((2, m))
    anywhere = pl.BlockSpec(memory_space=pl.ANY)
    local = pl.BlockSpec(memory_space=pltpu.VMEM)
    turned = lambda w: w.transpose(2, 3, 0, 1).reshape(-1, w.shape[1])
    operands = [
        frames.transpose(0, 2, 1, 3).reshape(n, 42, 8, 84),
        projection.T, hidden_state, cell_state, input_weight.reshape(4 * share, width),
        recur_weight.reshape(4 * share, nt * share), conv_first.transpose(2, 3, 1, 0),
        conv_second.transpose(2, 3, 1, 0).reshape(144, 32), turned(conv_third), turned(res_first),
        turned(res_second), counts, slot_ids, reset_flags, gate_bias, head_weight,
    ]
    shapes = [
        jax.ShapeDtypeStruct((head_weight.shape[0], n), F32),
        jax.ShapeDtypeStruct((share, slots), F32),
        jax.ShapeDtypeStruct((share, slots), F32),
    ]
    results = pl.pallas_call(
        step,
        out_shape=shapes,
        in_specs=[anywhere] * 16,
        out_specs=[local, anywhere, anywhere],
        scratch_shapes=[pltpu.VMEM(a.shape, a.dtype) for a in operands[1:]] + [
            vm(42, n, 8, 84),
            vmf(2, 6, n * 8, 128), vm(512, 768), vm(384, 256), vm(768, 256),
            vm(1152, 256), vm(1152, 384), vm(1152, 384), vmf(2, 3872, 128), vm(4224, 256),
            vm(87, n, 768), vm(6 * n, 256), vm(45, n, 896), vm(24, n, 896),
            vm(11, n, 384), vm(13, n, 384), vm(13, n, 384),
            vm(12 * n, 512), vm(12 * n, 512), vm(24 * n, 256), vm(24 * n, 256), vm(63 * n, 256),
            vmf(nd, 1, width), vmf(nd, 1, width), vm(nt, per, width), vmf(nt, per, 128),
            vmf(nt, per, 128), vmf(nd, 1, 128), vmf(nd, 1, 128), vmf(4 * share, rows),
            pairs(nd), pairs(nt), pairs(nt), pairs(nd),
            vmf(share, slots), vmf(share, slots), vm(nt, share, rows),
            pltpu.SemaphoreType.DMA((42,)), pltpu.SemaphoreType.DMA((15,)), pairs(nt),
            pltpu.SemaphoreType.DMA((2,)),
        ],
        compiler_params=pltpu.CompilerParams(
            vmem_limit_bytes=60 * 1024 * 1024, collective_id=0, has_side_effects=True
        ),
    )(*operands)
    return pl.pallas_call(
        hand_over, out_shape=shapes, in_specs=[local] * 3, out_specs=[local] * 3
    )(*results)


def solution(mesh):
    return jax.shard_map(
        body,
        mesh=mesh,
        in_specs=(
            P(("dp", "tensor"), None, None, None),
            P(),
            P("dp", None),
            P("dp", None),
            P("tensor", "dp"),
            P("tensor", "dp"),
            P(),
            P(),
            P(),
            P(),
            P(),
            P(),
            P(None, "tensor", None),
            P(None, "tensor", None),
            P(None, "tensor"),
            P(None, "tensor"),
        ),
        out_specs=(P(None, ("dp", "tensor")), P("tensor", "dp"), P("tensor", "dp")),
        check_vma=False,
    )
```

```python
import jax
import jax.numpy as jnp
from jax import lax
from jax.experimental import pallas as pl
from jax.experimental.pallas import tpu as pltpu
from jax.sharding import PartitionSpec as P

BF = jnp.bfloat16
F32 = jnp.float32
NEG = -3.0e38


def lanes(shape, dim):
    return lax.broadcasted_iota(jnp.int32, shape, dim)


def dot(a, b):
    return jnp.dot(a, b, preferred_element_type=F32)


def spread(w, width):
    pick = (lanes((width, 128), 1) % width == lanes((width, 128), 0)).astype(BF)
    return dot(w, pick)


def spread_turned(w):
    pick = (lanes((32, 128), 1) % 32 == lanes((32, 128), 0)).astype(BF)
    return jnp.concatenate(
        [
            lax.dot_general(
                w[k * 32 : k * 32 + 32, :], pick, (((0,), (0,)), ((), ())), preferred_element_type=F32
            )
            for k in range(9)
        ],
        axis=0,
    )


def band_weights(out_ref, tiled, depth, spots, per_lane, columns, first):
    width = 128 // per_lane
    lane = lanes((depth, 128), 1) // width
    for ky in range(3):
        for p in range(spots):
            for col in range(columns):
                block = None
                for i in range(per_lane):
                    start = first(col, i)
                    if start is None:
                        continue
                    kx = p - start
                    if 0 <= kx <= 2:
                        row = (ky * 3 + kx) * depth
                        part = jnp.where(lane == i, tiled[row : row + depth], 0.0)
                        block = part if block is None else block + part
                if block is None:
                    block = jnp.zeros((depth, 128), F32)
                row = (ky * spots + p) * depth
                out_ref[row : row + depth, col * 128 : col * 128 + 128] = block.astype(BF)


def column_mask(n, test):
    return jnp.where(test(lanes((n, 128), 1)), 1.0, 0.0).astype(BF)


def shifted(parts, pitch):
    inside = column_mask(parts[0].shape[0], lambda lane: lane < 128 - pitch) > 0.5
    rolled = [pltpu.roll(a, 128 - pitch, 1) for a in parts]
    return [
        jnp.where(inside, rolled[v], rolled[min(v + 1, len(parts) - 1)])
        for v in range(len(parts))
    ]


def alternate(count, produce, consume):
    produce(0, 0)

    def body(i, _):
        produce(2 * i + 1, 1)
        consume(2 * i, 0)
        produce(2 * i + 2, 0)
        consume(2 * i + 1, 1)
        return 0

    lax.fori_loop(0, (count - 1) // 2, body, 0)
    consume(count - 1, 0)


def count_tables(counts, me_t, me_d, cap, per):
    nd = counts.shape[1]
    own = counts[pl.ds(me_t, 1), :].astype(F32)
    a_row = lanes((nd, nd), 1)
    a_col = lanes((nd, nd), 0)
    wide = jnp.broadcast_to(own, (nd, nd))
    start_col = jnp.sum(jnp.where(a_row < a_col, wide, 0.0), axis=1, keepdims=True)
    count_col = jnp.sum(jnp.where(a_row == a_col, wide, 0.0), axis=1, keepdims=True)
    start_row = jnp.sum(
        jnp.where(a_col < a_row, jnp.broadcast_to(count_col, (nd, nd)), 0.0), axis=0, keepdims=True
    )
    mine = lanes((1, nd), 1) == me_d
    start = jnp.sum(jnp.where(mine, start_row, 0.0), axis=1, keepdims=True).astype(jnp.int32)
    count = jnp.sum(jnp.where(mine, own, 0.0), axis=1, keepdims=True).astype(jnp.int32)
    b, j = lanes((nd, cap), 0), lanes((nd, cap), 1)
    send = (jnp.bitwise_and(b - start - j, nd - 1) == 0) & (j < count)
    rank = (lanes((per, nd), 0) * nd + me_d).astype(F32)
    take = (start_row <= rank) & (rank < start_row + own)
    rank = (lanes((nd, per), 1) * nd + me_d).astype(F32)
    give = (start_col <= rank) & (rank < start_col + count_col)
    j, b = lanes((cap, nd), 0), lanes((cap, nd), 1)
    home = (jnp.bitwise_and(b - start - j, nd - 1) == 0) & (j < count)
    as_f32 = lambda m: jnp.where(m, 1.0, 0.0)
    return as_f32(send), as_f32(take), as_f32(give), as_f32(home)


def dot_nt(a, b):
    return lax.dot_general(a, b, (((1,), (1,)), ((), ())), preferred_element_type=F32)


def chosen_rows(a, b, turn=False):
    value, pick = (a, b.astype(BF)) if turn else (b, a.astype(BF))
    high = value.astype(BF)
    rest = value - high.astype(F32)
    middle = rest.astype(BF)
    terms = (high, middle, (rest - middle.astype(F32)).astype(BF))
    parts = [dot(t, pick) if turn else dot(pick, t) for t in terms]
    return parts[0] + parts[1] + parts[2]


class Ring:
    def __init__(self, axis, other):
        self.axis, self.size, self.me = axis, lax.axis_size(axis), lax.axis_index(axis)
        self.other = lax.axis_index(other)

    def place(self, peer):
        return (peer, self.other) if self.axis == "dp" else (self.other, peer)

    def each(self, act):
        def step(i, _):
            k = 1 + lax.rem(i + self.size * 3 // 8, self.size - 1)
            act(k, jnp.bitwise_and(self.me + k, self.size - 1))
            return 0

        lax.fori_loop(0, self.size - 1, step, 0, unroll=True)

    def copy(self, k, peer, src, dst, sems):
        return pltpu.make_async_remote_copy(
            src_ref=src, dst_ref=dst, send_sem=sems.at[0, k], recv_sem=sems.at[1, k],
            device_id=self.place(peer), device_id_type=pl.DeviceIdType.MESH,
        )


def greet(rings):
    barrier = pltpu.get_barrier_semaphore()
    for ring in rings:
        ring.each(
            lambda k, peer, ring=ring: pl.semaphore_signal(
                barrier, inc=1, device_id=ring.place(peer), device_id_type=pl.DeviceIdType.MESH
            )
        )


def meet(rings):
    pl.semaphore_wait(pltpu.get_barrier_semaphore(), sum(ring.size - 1 for ring in rings))


def send_hidden(ring, ids, reset, hid, hall, sems):
    slots, rows = hid.shape[1], ids.shape[1]
    keep = (1 - reset[...]).astype(F32)
    pick = jnp.where(lanes((slots, rows), 0) == ids[...], 1.0, 0.0)
    hall[ring.me] = dot((hid[...] * keep).astype(BF), pick.astype(BF)).astype(BF)
    copy = lambda k, peer: ring.copy(k, peer, hall.at[ring.me], hall.at[ring.me], sems)
    ring.each(lambda k, peer: copy(k, peer).start())
    return copy


def core(
    feat, dp, tp, hidden_copy, waits, tables, stores,
    ids, reset, bias, head, hid, cell, win, wrec,
    out, hout, cout,
    hall, orow, inrow, fall, hp, hin, brow, rrow, gates, sem_f, sem_g, sem_h, sem_b,
):
    per = fall.shape[1]
    share, slots = hid.shape
    rows = ids.shape[1]
    send, take, give, home = tables

    spread_rows = dot(send.astype(BF), feat)
    for b in range(dp.size):
        orow[b] = spread_rows[b : b + 1]
    inrow[dp.me] = orow[dp.me]
    row_copy = lambda k, peer: dp.copy(k, peer, orow.at[peer], inrow.at[dp.me], sem_f)
    dp.each(lambda k, peer: row_copy(k, peer).start())

    waits()
    keep = (1 - reset[...]).astype(F32)
    pick = jnp.where(lanes((slots, rows), 0) == ids[...], 1.0, 0.0)
    tp.each(lambda k, peer: hidden_copy(k, peer).wait())
    everyone = hall[...].reshape(tp.size * share, rows)
    recurrent = []
    for q in range(4):
        tall = jnp.transpose(jnp.broadcast_to(bias[q : q + 1, :], (8, share)))[:, 0:1]
        gates[q * share : (q + 1) * share] = dot(wrec[q * share : (q + 1) * share], everyone) + tall
    prev_cell = chosen_rows(cell[...] * keep, pick, True)

    dp.each(lambda k, peer: row_copy(k, peer).wait())
    gathered = jnp.concatenate([inrow[a] for a in range(dp.size)], axis=0)
    fall[tp.me] = dot(take.astype(BF), gathered.astype(BF)).astype(BF)
    feat_copy = lambda k, peer: tp.copy(k, peer, fall.at[tp.me], fall.at[tp.me], sem_g)
    tp.each(lambda k, peer: feat_copy(k, peer).start())
    tp.each(lambda k, peer: feat_copy(k, peer).wait())

    features = fall[...].reshape(rows, fall.shape[2])
    sums = gates[...] + dot_nt(win[...], features)
    gate = [sums[q * share : (q + 1) * share] for q in range(4)]
    next_cell = jax.nn.sigmoid(gate[1]) * prev_cell + jax.nn.sigmoid(gate[0]) * jnp.tanh(gate[2])
    next_hidden = jax.nn.sigmoid(gate[3]) * jnp.tanh(next_cell)
    partial = jnp.transpose(dot(head[...], next_hidden.astype(BF)))
    width = partial.shape[1]
    for t in range(tp.size):
        hp[t, :, 0:width] = partial[t * per : (t + 1) * per]
    hin[tp.me] = hp[tp.me]
    sum_copy = lambda k, peer: tp.copy(k, peer, hp.at[peer], hin.at[tp.me], sem_h)
    tp.each(lambda k, peer: sum_copy(k, peer).start())

    square = lanes((rows, rows), 0) == lanes((rows, rows), 1)
    column = jnp.sum(jnp.where(square, ids[...], 0).astype(F32), axis=1, keepdims=True)
    lay = jnp.where(lanes((rows, slots), 1).astype(F32) == column, 1.0, 0.0)
    chosen = jnp.sum(lay, axis=0, keepdims=True) > 0.0
    hout[...] = jnp.where(chosen, chosen_rows(next_hidden, lay, True), hid[...])
    cout[...] = jnp.where(chosen, chosen_rows(next_cell, lay, True), cell[...])

    for store in stores:
        store.start()
    tp.each(lambda k, peer: sum_copy(k, peer).wait())
    total = hin[0]
    for t in range(1, tp.size):
        total = total + hin[t]
    back = chosen_rows(give, total)
    for a in range(dp.size):
        brow[a] = back[a : a + 1]
    rrow[dp.me] = brow[dp.me]
    back_copy = lambda k, peer: dp.copy(k, peer, brow.at[peer], rrow.at[dp.me], sem_b)
    dp.each(lambda k, peer: back_copy(k, peer).start())
    dp.each(lambda k, peer: back_copy(k, peer).wait())
    heads = chosen_rows(home, jnp.concatenate([rrow[a] for a in range(dp.size)], axis=0))
    out[...] = jnp.transpose(heads)[0 : out.shape[0], :]
    for store in stores:
        store.wait()


def encoder(
    fetch, ready, after_cut, w1, w2, w3, r1, r2, pt,
    raw, flat, sel, k1, k2, k3, kr1, kr2, ptf, ptk, u, carry, p1, p2, p3, p3r, q1,
    wide0, wide1, acc0, acc1, third,
):
    pairs, n = raw.shape[0:2]
    wide, acc = (wide0, wide1), (acc0, acc1)
    ready("conv")
    column = lanes((256, 384), 1)
    window, spot = column // 64, column % 64
    source = spot // 18 * 128 + window * 16 - 11 + spot % 18
    x = lanes((256, 384), 0)
    inside = (spot < 36) & (source // 128 == spot // 18) & (source >= 0)
    sel[...] = jnp.where(inside & (source == x), 1.0, 0.0).astype(BF)
    t1 = [spread(w1[k // 3, k % 3], 16) for k in range(9)]
    t1 = [jnp.concatenate([t, t], axis=1) for t in t1]
    row = lanes((128, 256), 0)
    spot = row % 40
    kx = spot % 18 - 2 * (lanes((128, 256), 1) // 16 % 8) - lanes((128, 256), 1) // 128
    code = jnp.where((kx >= 0) & (kx <= 2) & (spot < 36), row // 40 * 6 + spot // 18 * 3 + kx, -1)
    for pair in range(2):
        block = jnp.zeros((128, 256), F32)
        for ky in range(3):
            for c in range(2):
                for k in range(3):
                    line = t1[ky * 3 + k][pair * 2 + c : pair * 2 + c + 1]
                    block = jnp.where(code == ky * 6 + c * 3 + k, line, block)
        block = block.astype(BF)
        k1[0, pair * 128 : pair * 128 + 128] = block
        k1[1, pair * 128 : pair * 128 + 64] = block[64:]
        k1[1, pair * 128 + 64 : pair * 128 + 128] = block[:64]
    both = lambda col, i: 2 * i + col
    band_weights(k2, spread(w2[...], 32), 16, 16, 4, 2, both)
    band_weights(k3, spread_turned(w3), 32, 12, 4, 2, both)
    same = lambda col, i: None if col * 4 + i > 10 else col * 4 + i - 1
    band_weights(kr1, spread_turned(r1), 32, 12, 4, 3, same)
    band_weights(kr2, spread_turned(r2), 32, 12, 4, 3, same)

    ready("dense")

    def widen(i, _):
        rows = pl.ds(i * 352, 352)
        block = pt[rows, :].astype(F32)
        ptf[0, rows, :] = block[:, :128]
        ptf[1, rows, :] = block[:, 128:]
        return 0

    lax.fori_loop(0, 11, widen, 0)

    def reorder(y, _):
        for px in range(11):
            rows = pl.ds(y * 384 + px * 32, 32)
            for h in range(2):
                ptk[rows, h * 128 : h * 128 + 128] = ptf[
                    h, pl.ds(y * 11 + px, 32, stride=121), :
                ].astype(BF)
        ptk[pl.ds(y * 384 + 352, 32), :] = jnp.zeros((32, 256), BF)
        return 0

    lax.fori_loop(0, 11, reorder, 0)

    for r in range(3):
        for y in (0, 2 * pairs + 1, 2 * pairs + 2):
            u[r, y] = jnp.zeros((2, n, 384), BF)
    p1[0] = jnp.zeros((n, 896), BF)
    p1[43] = jnp.zeros((n, 896), BF)
    p1[44] = jnp.zeros((n, 896), BF)
    p2[0] = jnp.zeros((n, 896), BF)
    p2[22] = jnp.zeros((n, 896), BF)
    p2[23] = jnp.zeros((n, 896), BF)
    for ref in (p3r, q1):
        ref[0] = jnp.zeros((n, 384), BF)
        ref[12] = jnp.zeros((n, 384), BF)
    flat[...] = jnp.zeros_like(flat)

    batch = 6

    def unpack(i, slot):
        for g in range(batch):
            q = i * batch + g
            fetch(q).wait()
            flat[slot, g, :, 0:84] = raw[q].astype(F32).reshape(n * 8, 84)
        for g in range(batch):
            for y in range(2):
                for c in range(4):
                    line = ((c // 2 * batch + g) * 2 + y) * n
                    wide[slot][line : line + n, c % 2 * 128 : c % 2 * 128 + 128] = flat[
                        slot, g, pl.ds(y * 4 + c, n, stride=8), :
                    ].astype(BF)

    def cut(i, slot):
        got = dot(wide[slot][...], sel[...]).astype(BF)
        size = 2 * batch * n
        for pair in range(2):
            for v in range(3):
                part = got[pair * size : pair * size + size, v * 128 : v * 128 + 128]
                for r in range(3):
                    moved = pltpu.roll(part, 40 * r, 1) if r else part
                    u[r, pl.ds(i * 2 * batch + 1, 2 * batch), pair, :, v * 128 : v * 128 + 128] = (
                        moved.reshape(2 * batch, n, 128)
                    )

    alternate(pairs // batch, unpack, cut)
    after_cut()

    lane_in = lambda a, b: column_mask(n, lambda lane: (lane >= a) & (lane < b)) > 0.5
    ranges = (
        (lane_in(0, 40), lane_in(40, 80)),
        (lane_in(64, 104), column_mask(n, lambda lane: (lane >= 104) | (lane < 16)) > 0.5),
    )

    def first_conv(target, y, rows):
        lhs = ([], [])
        for r in range(rows):
            for v in range(3):
                packed = ([], [])
                for pair in range(2):
                    a, b, c = (
                        u[ky, y + r + ky, pair, :, v * 128 : v * 128 + 128] for ky in range(3)
                    )
                    for odd in range(2):
                        at_a, at_b = ranges[odd]
                        packed[odd].append(jnp.where(at_a, a, jnp.where(at_b, b, c)))
                for odd in range(2):
                    lhs[odd].append(jnp.concatenate(packed[odd], axis=1))
        for odd in range(2):
            got = dot(jnp.concatenate(lhs[odd], axis=0), k1[odd]).astype(BF)
            for r in range(rows):
                for v in range(3):
                    line = (r * 6 + 2 * v + odd) * n
                    target[line : line + n] = got[(r * 3 + v) * n : (r * 3 + v + 1) * n]

    def conv_row(src, y, count, step, width):
        taps = [src[y + ky] for ky in range(3)]
        return [
            jnp.concatenate([t[:, v * step : v * step + width] for t in taps], axis=1)
            for v in range(count)
        ]

    def conv_rows(src, y, rows, count, step, width, weights):
        lhs = [a for r in range(rows) for a in conv_row(src, y + r, count, step, width)]
        return dot(jnp.concatenate(lhs, axis=0), weights[...]).astype(BF)

    zero = jnp.zeros((), BF)

    def second_conv(target, y, rows):
        target[0 : rows * 6 * n] = conv_rows(p1, y, rows, 6, 128, 256, k2)

    def pool_stage(conv, dst, group, count, per, pitch, offset, limit, last):
        size = count * n
        conv(carry, 0, 1)
        first = column_mask(n, lambda lane: lane // pitch >= offset) > 0.5
        final = column_mask(
            n, lambda lane: lane // pitch + ((count - 1) * per - offset) < limit
        ) > 0.5

        def produce(i, slot):
            conv(acc[slot], 2 * group * i + 1, 2 * group)

        def consume(i, slot):
            for g in range(group):
                y = i * group + g
                row = lambda r, v, h: acc[slot][
                    r * size + v * n : r * size + v * n + n, h * 128 : h * 128 + 128
                ]
                keep = jnp.where(y < last, 1.0, 0.0).astype(BF) if g == group - 1 else None
                half = []
                for h in range(2):
                    tops = []
                    for v in range(count):
                        now, later = row(2 * g, v, h), row(2 * g + 1, v, h)
                        if keep is not None:
                            later = later * keep
                        if g == 0:
                            before = carry[v * n : v * n + n, h * 128 : h * 128 + 128]
                        else:
                            before = row(2 * g - 1, v, h)
                        tops.append(jnp.maximum(jnp.maximum(before, now), jnp.maximum(later, zero)))
                        if g == group - 1:
                            carry[v * n : v * n + n, h * 128 : h * 128 + 128] = later
                    half.append(tops)
                even, odd = half
                even[-1] = jnp.where(final, even[-1], zero)
                nxt = shifted(even, pitch)
                for v in range(count):
                    best = jnp.maximum(jnp.maximum(even[v], odd[v]), nxt[v])
                    if v == 0:
                        best = jnp.where(first, best, zero)
                    if v == count - 1:
                        best = jnp.where(final, best, zero)
                    dst[y + 1, :, v * 128 : v * 128 + 128] = best
                dst[y + 1, :, count * 128 : count * 128 + 128] = jnp.zeros((n, 128), BF)

        alternate((last + 1) // group, produce, consume)

    pool_stage(first_conv, p1, 2, 6, 8, 16, 5, 42, 41)
    pool_stage(second_conv, p2, 1, 6, 4, 32, 2, 21, 20)

    for y in range(0, 21, 7):
        third[y * 3 * n : (y + 7) * 3 * n] = conv_rows(p2, y, 7, 3, 256, 384, k3)
    low = jnp.full((), NEG, BF)
    begin = column_mask(n, lambda lane: lane >= 32) > 0.5
    inner = column_mask(n, lambda lane: lane < 96) > 0.5
    for y in range(11):
        half = []
        for h in range(2):
            tops = []
            for v in range(3):
                top = None
                for r in range(max(2 * y - 1, 0), min(2 * y + 2, 21)):
                    at = (r * 3 + v) * n
                    part = third[at : at + n, h * 128 : h * 128 + 128]
                    top = part if top is None else jnp.maximum(top, part)
                tops.append(top)
            half.append(tops)
        even, odd = half
        even[0] = jnp.where(begin, even[0], low)
        even[2] = jnp.where(inner, even[2], low)
        nxt = shifted(even, 32)
        for v in range(3):
            best = jnp.maximum(jnp.maximum(even[v], odd[v]), nxt[v])
            if v == 2:
                best = jnp.where(inner, best, zero)
            p3[y, :, v * 128 : v * 128 + 128] = best
            p3r[y + 1, :, v * 128 : v * 128 + 128] = jnp.maximum(best, zero)

    def full_rows(src):
        return jnp.concatenate(
            [jnp.concatenate([src[y + ky] for ky in range(3)], axis=1) for y in range(11)], axis=0
        )

    q1[1:12] = jnp.maximum(dot(full_rows(p3r), kr1[...]), 0.0).astype(BF).reshape(11, n, 384)
    final = dot(full_rows(q1), kr2[...]) + p3[...].reshape(11 * n, 384).astype(F32)
    final = jnp.maximum(final, 0.0).astype(BF)
    line = jnp.concatenate([final[y * n : y * n + n] for y in range(11)], axis=1)
    return jnp.maximum(dot(line, ptk[...]), 0.0).astype(BF)


def step(*refs):
    hbm, (out, hout, cout) = refs[:16], refs[16:19]
    held, (raw, *enc), own = refs[19:34], refs[34:34 + 22], refs[34 + 22:46 + 22]
    hnew, cnew, hall, sem_q, sem_w, sem_x, sem_o = refs[46 + 22:]
    dp, tp = Ring("dp", "tensor"), Ring("tensor", "dp")
    frames = hbm[0]
    loads = [pltpu.make_async_copy(hbm[i + 1], held[i], sem_w.at[i]) for i in range(15)]
    names = ("pt", "hid", "cell", "win", "wrec", "w1", "w2", "w3", "r1", "r2")
    at = {name: i for i, name in enumerate(names + ("counts", "ids", "reset", "bias", "head"))}
    ref = lambda *which: [held[at[name]] for name in which]
    groups = {
        "conv": ("w1", "w2", "w3", "r1", "r2"),
        "dense": ("pt",),
        "hidden": ("hid", "counts", "ids", "reset"),
        "rest": ("cell", "win", "wrec", "bias", "head"),
    }

    def ready(group):
        for name in groups[group]:
            loads[at[name]].wait()

    def fetch(q):
        return pltpu.make_async_copy(frames.at[:, q], raw.at[q], sem_q.at[q])

    def start(q, _):
        fetch(q).start()
        return 0

    greet((dp, tp))
    for name in groups["conv"] + groups["hidden"]:
        loads[at[name]].start()
    lax.fori_loop(0, raw.shape[0], start, 0)
    for name in groups["dense"] + groups["rest"]:
        loads[at[name]].start()
    own[4][...] = jnp.zeros_like(own[4])
    sent = []
    counts, ids, reset, hid = ref("counts", "ids", "reset", "hid")

    def share_hidden():
        ready("hidden")
        sent.extend(count_tables(counts, tp.me, dp.me, frames.shape[0], own[2].shape[1]))
        meet((dp, tp))
        sent.append(send_hidden(tp, ids, reset, hid, hall, sem_x))

    feat = encoder(fetch, ready, share_hidden, *ref(*groups["conv"], "pt"), raw, *enc)
    stores = [
        pltpu.make_async_copy(hnew, hout, sem_o.at[0]),
        pltpu.make_async_copy(cnew, cout, sem_o.at[1]),
    ]
    core(
        feat, dp, tp, sent[4], lambda: ready("rest"), sent[0:4], stores, ids, reset,
        *ref("bias", "head", "hid", "cell", "win", "wrec"), out, hnew, cnew, hall, *own,
    )


def hand_over(*refs):
    given, results, held, sems = refs[0:3], refs[3:6], refs[6:9], refs[9]
    half = held[1].shape[0] // 2
    spans = [(0, pl.ds(0, held[0].shape[0]))]
    spans += [(i, pl.ds(k * half, half)) for k in range(2) for i in (1, 2)]
    moves = [
        [
            pltpu.make_async_copy(src[i].at[rows], dst[i].at[rows], sems.at[way, at])
            for way, (src, dst) in enumerate(((given, held), (held, results)))
        ]
        for at, (i, rows) in enumerate(spans)
    ]
    for inward, _ in moves:
        inward.start()
    for inward, outward in moves:
        inward.wait()
        outward.start()
    for _, outward in moves:
        outward.wait()


def body(
    frames, counts, slot_ids, reset_flags, hidden_state, cell_state, conv_first, conv_second,
    conv_third, res_first, res_second, projection, input_weight, recur_weight, gate_bias, head_weight,
):
    n = frames.shape[0]
    share, slots = hidden_state.shape
    nd, nt = lax.axis_size("dp"), lax.axis_size("tensor")
    rows = slot_ids.shape[1]
    per = rows // nt
    width = input_weight.shape[2]
    vm = lambda *s: pltpu.VMEM(s, BF)
    vmf = lambda *s: pltpu.VMEM(s, F32)
    pairs = lambda m: pltpu.SemaphoreType.DMA((2, m))
    anywhere = pl.BlockSpec(memory_space=pl.ANY)
    local = pl.BlockSpec(memory_space=pltpu.VMEM)
    turned = lambda w: w.transpose(2, 3, 0, 1).reshape(-1, w.shape[1])
    operands = [
        frames.transpose(0, 2, 1, 3).reshape(n, 42, 8, 84),
        projection.T, hidden_state, cell_state, input_weight.reshape(4 * share, width),
        recur_weight.reshape(4 * share, nt * share), conv_first.transpose(2, 3, 1, 0),
        conv_second.transpose(2, 3, 1, 0).reshape(144, 32), turned(conv_third), turned(res_first),
        turned(res_second), counts, slot_ids, reset_flags, gate_bias, head_weight,
    ]
    shapes = [
        jax.ShapeDtypeStruct((head_weight.shape[0], n), F32),
        jax.ShapeDtypeStruct((share, slots), F32),
        jax.ShapeDtypeStruct((share, slots), F32),
    ]
    results = pl.pallas_call(
        step,
        out_shape=shapes,
        in_specs=[anywhere] * 16,
        out_specs=[local, anywhere, anywhere],
        scratch_shapes=[pltpu.VMEM(a.shape, a.dtype) for a in operands[1:]] + [
            vm(42, n, 8, 84),
            vmf(2, 6, n * 8, 128), vm(256, 384), vm(2, 256, 256), vm(768, 256),
            vm(1152, 256), vm(1152, 384), vm(1152, 384), vmf(2, 3872, 128), vm(4224, 256),
            vm(3, 87, 2, n, 384), vm(6 * n, 256), vm(45, n, 896), vm(24, n, 896),
            vm(11, n, 384), vm(13, n, 384), vm(13, n, 384),
            vm(24 * n, 256), vm(24 * n, 256), vm(24 * n, 256), vm(24 * n, 256), vm(63 * n, 256),
            vmf(nd, 1, width), vmf(nd, 1, width), vm(nt, per, width), vmf(nt, per, 128),
            vmf(nt, per, 128), vmf(nd, 1, 128), vmf(nd, 1, 128), vmf(4 * share, rows),
            pairs(nd), pairs(nt), pairs(nt), pairs(nd),
            vmf(share, slots), vmf(share, slots), vm(nt, share, rows),
            pltpu.SemaphoreType.DMA((42,)), pltpu.SemaphoreType.DMA((15,)), pairs(nt),
            pltpu.SemaphoreType.DMA((2,)),
        ],
        compiler_params=pltpu.CompilerParams(
            vmem_limit_bytes=60 * 1024 * 1024, collective_id=0, has_side_effects=True
        ),
    )(*operands)
    return pl.pallas_call(
        hand_over,
        out_shape=shapes,
        in_specs=[anywhere] * 3,
        out_specs=[anywhere] * 3,
        scratch_shapes=[pltpu.VMEM(a.shape, a.dtype) for a in shapes]
        + [pltpu.SemaphoreType.DMA((2, 5))],
    )(*results)


def solution(mesh):
    return jax.shard_map(
        body,
        mesh=mesh,
        in_specs=(
            P(("dp", "tensor"), None, None, None),
            P(),
            P("dp", None),
            P("dp", None),
            P("tensor", "dp"),
            P("tensor", "dp"),
            P(),
            P(),
            P(),
            P(),
            P(),
            P(),
            P(None, "tensor", None),
            P(None, "tensor", None),
            P(None, "tensor"),
            P(None, "tensor"),
        ),
        out_specs=(P(None, ("dp", "tensor")), P("tensor", "dp"), P("tensor", "dp")),
        check_vma=False,
    )
```

```python
import jax
import jax.numpy as jnp
from jax import lax
from jax.experimental import pallas as pl
from jax.experimental.pallas import tpu as pltpu
from jax.sharding import PartitionSpec as P

BF = jnp.bfloat16
F32 = jnp.float32
NEG = -3.0e38


def lanes(shape, dim):
    return lax.broadcasted_iota(jnp.int32, shape, dim)


def dot(a, b):
    return jnp.dot(a, b, preferred_element_type=F32)


def spread(w, width):
    pick = (lanes((width, 128), 1) % width == lanes((width, 128), 0)).astype(BF)
    return dot(w, pick)


def spread_turned(w):
    pick = (lanes((32, 128), 1) % 32 == lanes((32, 128), 0)).astype(BF)
    return jnp.concatenate(
        [
            lax.dot_general(
                w[k * 32 : k * 32 + 32, :], pick, (((0,), (0,)), ((), ())), preferred_element_type=F32
            )
            for k in range(9)
        ],
        axis=0,
    )


def band_weights(out_ref, tiled, depth, spots, per_lane, columns, first, place=None):
    width = 128 // per_lane
    lane = lanes((depth, 128), 1) // width
    for ky in range(3):
        for p in range(spots):
            for col in range(columns):
                block = None
                for i in range(per_lane):
                    start = first(col, i)
                    if start is None:
                        continue
                    kx = p - start
                    if 0 <= kx <= 2:
                        row = (ky * 3 + kx) * depth
                        part = jnp.where(lane == i, tiled[row : row + depth], 0.0)
                        block = part if block is None else block + part
                if block is None:
                    block = jnp.zeros((depth, 128), F32)
                row = (ky * spots + p) * depth if place is None else place(ky, p)
                out_ref[row : row + depth, col * 128 : col * 128 + 128] = block.astype(BF)


def column_mask(n, test):
    return jnp.where(test(lanes((n, 128), 1)), 1.0, 0.0).astype(BF)


def shifted(parts, pitch):
    inside = column_mask(parts[0].shape[0], lambda lane: lane < 128 - pitch) > 0.5
    rolled = [pltpu.roll(a, 128 - pitch, 1) for a in parts]
    return [
        jnp.where(inside, rolled[v], rolled[min(v + 1, len(parts) - 1)])
        for v in range(len(parts))
    ]


def alternate(count, produce, consume):
    produce(0, 0)

    def body(i, _):
        produce(2 * i + 1, 1)
        consume(2 * i, 0)
        produce(2 * i + 2, 0)
        consume(2 * i + 1, 1)
        return 0

    lax.fori_loop(0, (count - 1) // 2, body, 0)
    consume(count - 1, 0)


def count_tables(counts, me_t, me_d, cap, per):
    nd = counts.shape[1]
    own = counts[pl.ds(me_t, 1), :].astype(F32)
    a_row = lanes((nd, nd), 1)
    a_col = lanes((nd, nd), 0)
    wide = jnp.broadcast_to(own, (nd, nd))
    start_col = jnp.sum(jnp.where(a_row < a_col, wide, 0.0), axis=1, keepdims=True)
    count_col = jnp.sum(jnp.where(a_row == a_col, wide, 0.0), axis=1, keepdims=True)
    start_row = jnp.sum(
        jnp.where(a_col < a_row, jnp.broadcast_to(count_col, (nd, nd)), 0.0), axis=0, keepdims=True
    )
    mine = lanes((1, nd), 1) == me_d
    start = jnp.sum(jnp.where(mine, start_row, 0.0), axis=1, keepdims=True).astype(jnp.int32)
    count = jnp.sum(jnp.where(mine, own, 0.0), axis=1, keepdims=True).astype(jnp.int32)
    b, j = lanes((nd, cap), 0), lanes((nd, cap), 1)
    send = (jnp.bitwise_and(b - start - j, nd - 1) == 0) & (j < count)
    rank = (lanes((per, nd), 0) * nd + me_d).astype(F32)
    take = (start_row <= rank) & (rank < start_row + own)
    rank = (lanes((nd, per), 1) * nd + me_d).astype(F32)
    give = (start_col <= rank) & (rank < start_col + count_col)
    j, b = lanes((cap, nd), 0), lanes((cap, nd), 1)
    home = (jnp.bitwise_and(b - start - j, nd - 1) == 0) & (j < count)
    as_f32 = lambda m: jnp.where(m, 1.0, 0.0)
    return as_f32(send), as_f32(take), as_f32(give), as_f32(home)


def dot_nt(a, b):
    return lax.dot_general(a, b, (((1,), (1,)), ((), ())), preferred_element_type=F32)


def chosen_rows(a, b, turn=False):
    value, pick = (a, b.astype(BF)) if turn else (b, a.astype(BF))
    high = value.astype(BF)
    rest = value - high.astype(F32)
    middle = rest.astype(BF)
    terms = (high, middle, (rest - middle.astype(F32)).astype(BF))
    parts = [dot(t, pick) if turn else dot(pick, t) for t in terms]
    return parts[0] + parts[1] + parts[2]


class Ring:
    def __init__(self, axis, other):
        self.axis, self.size, self.me = axis, lax.axis_size(axis), lax.axis_index(axis)
        self.other = lax.axis_index(other)

    def place(self, peer):
        return (peer, self.other) if self.axis == "dp" else (self.other, peer)

    def each(self, act):
        def step(i, _):
            k = 1 + lax.rem(i + self.size * 3 // 8, self.size - 1)
            act(k, jnp.bitwise_and(self.me + k, self.size - 1))
            return 0

        lax.fori_loop(0, self.size - 1, step, 0, unroll=True)

    def copy(self, k, peer, src, dst, sems):
        return pltpu.make_async_remote_copy(
            src_ref=src, dst_ref=dst, send_sem=sems.at[0], recv_sem=sems.at[1],
            device_id=self.place(peer), device_id_type=pl.DeviceIdType.MESH,
        )


    def finish(self, ref, sems):
        others = ref.at[pl.ds(0, self.size - 1)]
        for way in range(2):
            pltpu.make_async_copy(others, others, sems.at[way]).wait()


def greet(rings):
    barrier = pltpu.get_barrier_semaphore()
    for ring in rings:
        ring.each(
            lambda k, peer, ring=ring: pl.semaphore_signal(
                barrier, inc=1, device_id=ring.place(peer), device_id_type=pl.DeviceIdType.MESH
            )
        )


def meet(rings):
    pl.semaphore_wait(pltpu.get_barrier_semaphore(), sum(ring.size - 1 for ring in rings))


def send_hidden(ring, ids, reset, hid, hall, sems):
    slots, rows = hid.shape[1], ids.shape[1]
    keep = (1 - reset[...]).astype(F32)
    pick = jnp.where(lanes((slots, rows), 0) == ids[...], 1.0, 0.0)
    hall[ring.me] = dot((hid[...] * keep).astype(BF), pick.astype(BF)).astype(BF)
    copy = lambda k, peer: ring.copy(k, peer, hall.at[ring.me], hall.at[ring.me], sems)
    ring.each(lambda k, peer: copy(k, peer).start())


def core(
    feat, dp, tp, hidden_sems, waits, tables, stores,
    ids, reset, bias, head, hid, cell, win, wrec,
    out, hout, cout,
    hall, orow, inrow, fall, hp, hin, brow, rrow, gates, sem_f, sem_g, sem_h, sem_b,
):
    per = fall.shape[1]
    share, slots = hid.shape
    rows = ids.shape[1]
    send, take, give, home = tables

    spread_rows = dot(send.astype(BF), feat)
    for b in range(dp.size):
        orow[b] = spread_rows[b : b + 1]
    inrow[dp.me] = orow[dp.me]
    row_copy = lambda k, peer: dp.copy(k, peer, orow.at[peer], inrow.at[dp.me], sem_f)
    dp.each(lambda k, peer: row_copy(k, peer).start())

    waits()
    keep = (1 - reset[...]).astype(F32)
    pick = jnp.where(lanes((slots, rows), 0) == ids[...], 1.0, 0.0)
    tp.finish(hall, hidden_sems)
    everyone = hall[...].reshape(tp.size * share, rows)
    recurrent = []
    for q in range(4):
        tall = jnp.transpose(jnp.broadcast_to(bias[q : q + 1, :], (8, share)))[:, 0:1]
        gates[q * share : (q + 1) * share] = dot(wrec[q * share : (q + 1) * share], everyone) + tall
    prev_cell = chosen_rows(cell[...] * keep, pick, True)

    dp.finish(inrow, sem_f)
    gathered = jnp.concatenate([inrow[a] for a in range(dp.size)], axis=0)
    fall[tp.me] = dot(take.astype(BF), gathered.astype(BF)).astype(BF)
    feat_copy = lambda k, peer: tp.copy(k, peer, fall.at[tp.me], fall.at[tp.me], sem_g)
    tp.each(lambda k, peer: feat_copy(k, peer).start())
    tp.finish(fall, sem_g)

    features = fall[...].reshape(rows, fall.shape[2])
    sums = gates[...] + dot_nt(win[...], features)
    gate = [sums[q * share : (q + 1) * share] for q in range(4)]
    next_cell = jax.nn.sigmoid(gate[1]) * prev_cell + jax.nn.sigmoid(gate[0]) * jnp.tanh(gate[2])
    next_hidden = jax.nn.sigmoid(gate[3]) * jnp.tanh(next_cell)
    partial = jnp.transpose(dot(head[...], next_hidden.astype(BF)))
    width = partial.shape[1]
    for t in range(tp.size):
        hp[t, :, 0:width] = partial[t * per : (t + 1) * per]
    hin[tp.me] = hp[tp.me]
    sum_copy = lambda k, peer: tp.copy(k, peer, hp.at[peer], hin.at[tp.me], sem_h)
    tp.each(lambda k, peer: sum_copy(k, peer).start())

    square = lanes((rows, rows), 0) == lanes((rows, rows), 1)
    column = jnp.sum(jnp.where(square, ids[...], 0).astype(F32), axis=1, keepdims=True)
    lay = jnp.where(lanes((rows, slots), 1).astype(F32) == column, 1.0, 0.0)
    chosen = jnp.sum(lay, axis=0, keepdims=True) > 0.0
    hout[...] = jnp.where(chosen, chosen_rows(next_hidden, lay, True), hid[...])
    cout[...] = jnp.where(chosen, chosen_rows(next_cell, lay, True), cell[...])

    for store in stores:
        store.start()
    tp.finish(hin, sem_h)
    total = hin[0]
    for t in range(1, tp.size):
        total = total + hin[t]
    back = chosen_rows(give, total)
    for a in range(dp.size):
        brow[a] = back[a : a + 1]
    rrow[dp.me] = brow[dp.me]
    back_copy = lambda k, peer: dp.copy(k, peer, brow.at[peer], rrow.at[dp.me], sem_b)
    dp.each(lambda k, peer: back_copy(k, peer).start())
    dp.finish(rrow, sem_b)
    heads = chosen_rows(home, jnp.concatenate([rrow[a] for a in range(dp.size)], axis=0))
    out[...] = jnp.transpose(heads)[0 : out.shape[0], :]
    for store in stores:
        store.wait()


def encoder(
    fetch, ready, after_cut, w1, w2, w3, r1, r2, pt,
    raw, flat, sel, k1, k2, k3, kr1, kr2, ptf, ptk, u, carry, p1, p2, p3, p3r, q1,
    wide0, wide1, acc0, acc1, third,
):
    pairs, n = raw.shape[0:2]
    wide, acc = (wide0, wide1), (acc0, acc1)
    ready("conv")
    column = lanes((256, 384), 1)
    window, spot = column // 64, column % 64
    source = spot // 18 * 128 + window * 16 - 11 + spot % 18
    x = lanes((256, 384), 0)
    inside = (spot < 36) & (source // 128 == spot // 18) & (source >= 0)
    sel[...] = jnp.where(inside & (source == x), 1.0, 0.0).astype(BF)
    t1 = [spread(w1[k // 3, k % 3], 16) for k in range(9)]
    t1 = [jnp.concatenate([t, t], axis=1) for t in t1]
    row = lanes((128, 256), 0)
    spot = row % 40
    kx = spot % 18 - 2 * (lanes((128, 256), 1) // 16 % 8) - lanes((128, 256), 1) // 128
    code = jnp.where((kx >= 0) & (kx <= 2) & (spot < 36), row // 40 * 6 + spot // 18 * 3 + kx, -1)
    for pair in range(2):
        block = jnp.zeros((128, 256), F32)
        for ky in range(3):
            for c in range(2):
                for k in range(3):
                    line = t1[ky * 3 + k][pair * 2 + c : pair * 2 + c + 1]
                    block = jnp.where(code == ky * 6 + c * 3 + k, line, block)
        block = block.astype(BF)
        k1[0, pair * 128 : pair * 128 + 128] = block
        k1[1, pair * 128 : pair * 128 + 64] = block[64:]
        k1[1, pair * 128 + 64 : pair * 128 + 128] = block[:64]
    both = lambda col, i: 2 * i + col
    tail = lambda ky, p: ky * 128 + p * 16 if p < 8 else 384 + ky * 32 + (p - 8) * 16
    band_weights(k2, spread(w2[...], 32), 16, 10, 4, 2, both, tail)
    k2[480:512] = jnp.zeros((32, 256), BF)
    band_weights(k3, spread_turned(w3), 32, 12, 4, 2, both)
    same = lambda col, i: None if col * 4 + i > 10 else col * 4 + i - 1
    band_weights(kr1, spread_turned(r1), 32, 12, 4, 3, same)
    band_weights(kr2, spread_turned(r2), 32, 12, 4, 3, same)

    ready("dense")

    def widen(i, _):
        rows = pl.ds(i * 352, 352)
        block = pt[rows, :].astype(F32)
        ptf[0, rows, :] = block[:, :128]
        ptf[1, rows, :] = block[:, 128:]
        return 0

    lax.fori_loop(0, 11, widen, 0)

    def reorder(y, _):
        for px in range(11):
            rows = pl.ds(y * 384 + px * 32, 32)
            for h in range(2):
                ptk[rows, h * 128 : h * 128 + 128] = ptf[
                    h, pl.ds(y * 11 + px, 32, stride=121), :
                ].astype(BF)
        ptk[pl.ds(y * 384 + 352, 32), :] = jnp.zeros((32, 256), BF)
        return 0

    lax.fori_loop(0, 11, reorder, 0)

    for r in range(3):
        for y in (0, 2 * pairs + 1, 2 * pairs + 2):
            u[r, y] = jnp.zeros((2, n, 384), BF)
    for r in range(3):
        for y in (0, 43, 44):
            p1[r, y] = jnp.zeros((n, 896), BF)
    p2[0, 0] = jnp.zeros((n, 896), BF)
    p2[0, 22] = jnp.zeros((n, 896), BF)
    p2[0, 23] = jnp.zeros((n, 896), BF)
    for ref in (p3r, q1):
        ref[0] = jnp.zeros((n, 384), BF)
        ref[12] = jnp.zeros((n, 384), BF)
    flat[...] = jnp.zeros_like(flat)

    batch = 6

    def unpack(i, slot):
        for g in range(batch):
            q = i * batch + g
            fetch(q).wait()
            flat[slot, g, :, 0:84] = raw[q].astype(F32).reshape(n * 8, 84)
        for g in range(batch):
            for y in range(2):
                for c in range(4):
                    line = ((c // 2 * batch + g) * 2 + y) * n
                    wide[slot][line : line + n, c % 2 * 128 : c % 2 * 128 + 128] = flat[
                        slot, g, pl.ds(y * 4 + c, n, stride=8), :
                    ].astype(BF)

    def cut(i, slot):
        got = dot(wide[slot][...], sel[...]).astype(BF)
        size = 2 * batch * n
        for pair in range(2):
            for v in range(3):
                part = got[pair * size : pair * size + size, v * 128 : v * 128 + 128]
                for r in range(3):
                    moved = pltpu.roll(part, 40 * r, 1) if r else part
                    u[r, pl.ds(i * 2 * batch + 1, 2 * batch), pair, :, v * 128 : v * 128 + 128] = (
                        moved.reshape(2 * batch, n, 128)
                    )

    alternate(pairs // batch, unpack, cut)
    after_cut()

    lane_in = lambda a, b: column_mask(n, lambda lane: (lane >= a) & (lane < b)) > 0.5
    ranges = (
        (lane_in(0, 40), lane_in(40, 80)),
        (lane_in(64, 104), column_mask(n, lambda lane: (lane >= 104) | (lane < 16)) > 0.5),
    )

    def first_conv(target, y, rows):
        lhs = ([], [])
        for r in range(rows):
            for v in range(3):
                packed = ([], [])
                for pair in range(2):
                    a, b, c = (
                        u[ky, y + r + ky, pair, :, v * 128 : v * 128 + 128] for ky in range(3)
                    )
                    for odd in range(2):
                        at_a, at_b = ranges[odd]
                        packed[odd].append(jnp.where(at_a, a, jnp.where(at_b, b, c)))
                for odd in range(2):
                    lhs[odd].append(jnp.concatenate(packed[odd], axis=1))
        for odd in range(2):
            got = dot(jnp.concatenate(lhs[odd], axis=0), k1[odd]).astype(BF)
            for r in range(rows):
                for v in range(3):
                    line = (r * 6 + 2 * v + odd) * n
                    target[line : line + n] = got[(r * 3 + v) * n : (r * 3 + v + 1) * n]

    def conv_row(src, y, count, step, width):
        taps = [src[y + ky] for ky in range(3)]
        return [
            jnp.concatenate([t[:, v * step : v * step + width] for t in taps], axis=1)
            for v in range(count)
        ]

    def conv_rows(src, y, rows, count, step, width, weights):
        lhs = [a for r in range(rows) for a in conv_row(src, y + r, count, step, width)]
        return dot(jnp.concatenate(lhs, axis=0), weights[...]).astype(BF)

    zero = jnp.zeros((), BF)

    end_a, end_b = lane_in(0, 32), lane_in(32, 64)

    def second_conv(target, y, rows):
        lhs = []
        for r in range(rows):
            for v in range(6):
                here, after = v * 128, v * 128 + 128
                main = [p1[0, y + r + ky, :, here : here + 128] for ky in range(3)]
                a, b, c = (p1[ky, y + r + ky, :, after : after + 128] for ky in range(3))
                ends = jnp.where(end_a, a, jnp.where(end_b, b, c))
                lhs.append(jnp.concatenate(main + [ends], axis=1))
        target[0 : rows * 6 * n] = dot(jnp.concatenate(lhs, axis=0), k2[...]).astype(BF)

    def pool_stage(conv, dst, group, count, per, pitch, offset, limit, last, copies):
        size = count * n
        conv(carry, 0, 1)
        first = column_mask(n, lambda lane: lane // pitch >= offset) > 0.5
        final = column_mask(
            n, lambda lane: lane // pitch + ((count - 1) * per - offset) < limit
        ) > 0.5

        def produce(i, slot):
            conv(acc[slot], 2 * group * i + 1, 2 * group)

        def consume(i, slot):
            for g in range(group):
                y = i * group + g
                row = lambda r, v, h: acc[slot][
                    r * size + v * n : r * size + v * n + n, h * 128 : h * 128 + 128
                ]
                keep = jnp.where(y < last, 1.0, 0.0).astype(BF) if g == group - 1 else None
                half = []
                for h in range(2):
                    tops = []
                    for v in range(count):
                        now, later = row(2 * g, v, h), row(2 * g + 1, v, h)
                        if keep is not None:
                            later = later * keep
                        if g == 0:
                            before = carry[v * n : v * n + n, h * 128 : h * 128 + 128]
                        else:
                            before = row(2 * g - 1, v, h)
                        tops.append(jnp.maximum(jnp.maximum(before, now), jnp.maximum(later, zero)))
                        if g == group - 1:
                            carry[v * n : v * n + n, h * 128 : h * 128 + 128] = later
                    half.append(tops)
                even, odd = half
                even[-1] = jnp.where(final, even[-1], zero)
                nxt = shifted(even, pitch)
                for v in range(count):
                    best = jnp.maximum(jnp.maximum(even[v], odd[v]), nxt[v])
                    if v == 0:
                        best = jnp.where(first, best, zero)
                    if v == count - 1:
                        best = jnp.where(final, best, zero)
                    for r in range(copies):
                        moved = pltpu.roll(best, 32 * r, 1) if r else best
                        dst[r, y + 1, :, v * 128 : v * 128 + 128] = moved
                for r in range(copies):
                    dst[r, y + 1, :, count * 128 : count * 128 + 128] = jnp.zeros((n, 128), BF)

        alternate((last + 1) // group, produce, consume)

    pool_stage(first_conv, p1, 6, 6, 8, 16, 5, 42, 41, 3)
    pool_stage(second_conv, p2, 3, 6, 4, 32, 2, 21, 20, 1)

    for y in range(0, 21, 7):
        third[y * 3 * n : (y + 7) * 3 * n] = conv_rows(p2.at[0], y, 7, 3, 256, 384, k3)
    low = jnp.full((), NEG, BF)
    begin = column_mask(n, lambda lane: lane >= 32) > 0.5
    inner = column_mask(n, lambda lane: lane < 96) > 0.5
    for y in range(11):
        half = []
        for h in range(2):
            tops = []
            for v in range(3):
                top = None
                for r in range(max(2 * y - 1, 0), min(2 * y + 2, 21)):
                    at = (r * 3 + v) * n
                    part = third[at : at + n, h * 128 : h * 128 + 128]
                    top = part if top is None else jnp.maximum(top, part)
                tops.append(top)
            half.append(tops)
        even, odd = half
        even[0] = jnp.where(begin, even[0], low)
        even[2] = jnp.where(inner, even[2], low)
        nxt = shifted(even, 32)
        for v in range(3):
            best = jnp.maximum(jnp.maximum(even[v], odd[v]), nxt[v])
            if v == 2:
                best = jnp.where(inner, best, zero)
            p3[y, :, v * 128 : v * 128 + 128] = best
            p3r[y + 1, :, v * 128 : v * 128 + 128] = jnp.maximum(best, zero)

    def full_rows(src):
        return jnp.concatenate(
            [jnp.concatenate([src[y + ky] for ky in range(3)], axis=1) for y in range(11)], axis=0
        )

    q1[1:12] = jnp.maximum(dot(full_rows(p3r), kr1[...]), 0.0).astype(BF).reshape(11, n, 384)
    final = dot(full_rows(q1), kr2[...]) + p3[...].reshape(11 * n, 384).astype(F32)
    final = jnp.maximum(final, 0.0).astype(BF)
    line = jnp.concatenate([final[y * n : y * n + n] for y in range(11)], axis=1)
    return jnp.maximum(dot(line, ptk[...]), 0.0).astype(BF)


def step(*refs):
    hbm, (out, hout, cout) = refs[:16], refs[16:19]
    held, (raw, *enc), own = refs[19:34], refs[34:34 + 22], refs[34 + 22:46 + 22]
    hnew, cnew, hall, sem_q, sem_w, sem_x, sem_o = refs[46 + 22:]
    dp, tp = Ring("dp", "tensor"), Ring("tensor", "dp")
    frames = hbm[0]
    loads = [pltpu.make_async_copy(hbm[i + 1], held[i], sem_w.at[i]) for i in range(15)]
    names = ("pt", "hid", "cell", "win", "wrec", "w1", "w2", "w3", "r1", "r2")
    at = {name: i for i, name in enumerate(names + ("counts", "ids", "reset", "bias", "head"))}
    ref = lambda *which: [held[at[name]] for name in which]
    groups = {
        "conv": ("w1", "w2", "w3", "r1", "r2"),
        "dense": ("pt",),
        "hidden": ("hid", "counts", "ids", "reset"),
        "rest": ("cell", "win", "wrec", "bias", "head"),
    }

    def ready(group):
        for name in groups[group]:
            loads[at[name]].wait()

    def fetch(q):
        return pltpu.make_async_copy(frames.at[:, q], raw.at[q], sem_q.at[q])

    def start(q, _):
        fetch(q).start()
        return 0

    greet((dp, tp))
    for name in groups["conv"] + groups["hidden"]:
        loads[at[name]].start()
    lax.fori_loop(0, raw.shape[0], start, 0)
    for name in groups["dense"] + groups["rest"]:
        loads[at[name]].start()
    own[4][...] = jnp.zeros_like(own[4])
    sent = []
    counts, ids, reset, hid = ref("counts", "ids", "reset", "hid")

    def share_hidden():
        ready("hidden")
        sent.extend(count_tables(counts, tp.me, dp.me, frames.shape[0], own[2].shape[1]))
        meet((dp, tp))
        send_hidden(tp, ids, reset, hid, hall, sem_x)

    feat = encoder(fetch, ready, share_hidden, *ref(*groups["conv"], "pt"), raw, *enc)
    stores = [
        pltpu.make_async_copy(hnew, hout, sem_o.at[0]),
        pltpu.make_async_copy(cnew, cout, sem_o.at[1]),
    ]
    core(
        feat, dp, tp, sem_x, lambda: ready("rest"), sent[0:4], stores, ids, reset,
        *ref("bias", "head", "hid", "cell", "win", "wrec"), out, hnew, cnew, hall, *own,
    )


def hand_over(*refs):
    given, results, held, sems = refs[0:3], refs[3:6], refs[6:9], refs[9]
    half = held[1].shape[0] // 2
    spans = [(0, pl.ds(0, held[0].shape[0]))]
    spans += [(i, pl.ds(k * half, half)) for k in range(2) for i in (1, 2)]
    moves = [
        [
            pltpu.make_async_copy(src[i].at[rows], dst[i].at[rows], sems.at[way, at])
            for way, (src, dst) in enumerate(((given, held), (held, results)))
        ]
        for at, (i, rows) in enumerate(spans)
    ]
    for inward, _ in moves:
        inward.start()
    for inward, outward in moves:
        inward.wait()
        outward.start()
    for _, outward in moves:
        outward.wait()


def body(
    frames, counts, slot_ids, reset_flags, hidden_state, cell_state, conv_first, conv_second,
    conv_third, res_first, res_second, projection, input_weight, recur_weight, gate_bias, head_weight,
):
    n = frames.shape[0]
    share, slots = hidden_state.shape
    nd, nt = lax.axis_size("dp"), lax.axis_size("tensor")
    rows = slot_ids.shape[1]
    per = rows // nt
    width = input_weight.shape[2]
    vm = lambda *s: pltpu.VMEM(s, BF)
    vmf = lambda *s: pltpu.VMEM(s, F32)
    pair = pltpu.SemaphoreType.DMA((2,))
    anywhere = pl.BlockSpec(memory_space=pl.ANY)
    local = pl.BlockSpec(memory_space=pltpu.VMEM)
    turned = lambda w: w.transpose(2, 3, 0, 1).reshape(-1, w.shape[1])
    operands = [
        frames.transpose(0, 2, 1, 3).reshape(n, 42, 8, 84),
        projection.T, hidden_state, cell_state, input_weight.reshape(4 * share, width),
        recur_weight.reshape(4 * share, nt * share), conv_first.transpose(2, 3, 1, 0),
        conv_second.transpose(2, 3, 1, 0).reshape(144, 32), turned(conv_third), turned(res_first),
        turned(res_second), counts, slot_ids, reset_flags, gate_bias, head_weight,
    ]
    shapes = [
        jax.ShapeDtypeStruct((head_weight.shape[0], n), F32),
        jax.ShapeDtypeStruct((share, slots), F32),
        jax.ShapeDtypeStruct((share, slots), F32),
    ]
    results = pl.pallas_call(
        step,
        out_shape=shapes,
        in_specs=[anywhere] * 16,
        out_specs=[local, anywhere, anywhere],
        scratch_shapes=[pltpu.VMEM(a.shape, a.dtype) for a in operands[1:]] + [
            vm(42, n, 8, 84),
            vmf(2, 6, n * 8, 128), vm(256, 384), vm(2, 256, 256), vm(512, 256),
            vm(1152, 256), vm(1152, 384), vm(1152, 384), vmf(2, 3872, 128), vm(4224, 256),
            vm(3, 87, 2, n, 384), vm(6 * n, 256), vm(3, 45, n, 896), vm(1, 24, n, 896),
            vm(11, n, 384), vm(13, n, 384), vm(13, n, 384),
            vm(24 * n, 256), vm(24 * n, 256), vm(72 * n, 256), vm(72 * n, 256), vm(63 * n, 256),
            vmf(nd, 1, width), vmf(nd, 1, width), vm(nt, per, width), vmf(nt, per, 128),
            vmf(nt, per, 128), vmf(nd, 1, 128), vmf(nd, 1, 128), vmf(4 * share, rows),
            pair, pair, pair, pair,
            vmf(share, slots), vmf(share, slots), vm(nt, share, rows),
            pltpu.SemaphoreType.DMA((42,)), pltpu.SemaphoreType.DMA((15,)), pair, pair,
        ],
        compiler_params=pltpu.CompilerParams(
            vmem_limit_bytes=60 * 1024 * 1024, collective_id=0, has_side_effects=True
        ),
    )(*operands)
    return pl.pallas_call(
        hand_over,
        out_shape=shapes,
        in_specs=[anywhere] * 3,
        out_specs=[anywhere] * 3,
        scratch_shapes=[pltpu.VMEM(a.shape, a.dtype) for a in shapes]
        + [pltpu.SemaphoreType.DMA((2, 5))],
    )(*results)


def solution(mesh):
    return jax.shard_map(
        body,
        mesh=mesh,
        in_specs=(
            P(("dp", "tensor"), None, None, None),
            P(),
            P("dp", None),
            P("dp", None),
            P("tensor", "dp"),
            P("tensor", "dp"),
            P(),
            P(),
            P(),
            P(),
            P(),
            P(),
            P(None, "tensor", None),
            P(None, "tensor", None),
            P(None, "tensor"),
            P(None, "tensor"),
        ),
        out_specs=(P(None, ("dp", "tensor")), P("tensor", "dp"), P("tensor", "dp")),
        check_vma=False,
    )
```

```python
import jax
import jax.numpy as jnp
from jax import lax
from jax.experimental import pallas as pl
from jax.experimental.pallas import tpu as pltpu
from jax.sharding import PartitionSpec as P

BF = jnp.bfloat16
F32 = jnp.float32
NEG = -3.0e38


def lanes(shape, dim):
    return lax.broadcasted_iota(jnp.int32, shape, dim)


def dot(a, b):
    return jnp.dot(a, b, preferred_element_type=F32)


def spread(w, width):
    pick = (lanes((width, 128), 1) % width == lanes((width, 128), 0)).astype(BF)
    return dot(w, pick)


def spread_turned(w):
    pick = (lanes((32, 128), 1) % 32 == lanes((32, 128), 0)).astype(BF)
    return jnp.concatenate(
        [
            lax.dot_general(
                w[k * 32 : k * 32 + 32, :], pick, (((0,), (0,)), ((), ())), preferred_element_type=F32
            )
            for k in range(9)
        ],
        axis=0,
    )


def band_weights(out_ref, tiled, depth, spots, per_lane, columns, first, place=None):
    width = 128 // per_lane
    lane = lanes((depth, 128), 1) // width
    for ky in range(3):
        for p in range(spots):
            for col in range(columns):
                block = None
                for i in range(per_lane):
                    start = first(col, i)
                    if start is None:
                        continue
                    kx = p - start
                    if 0 <= kx <= 2:
                        row = (ky * 3 + kx) * depth
                        part = jnp.where(lane == i, tiled[row : row + depth], 0.0)
                        block = part if block is None else block + part
                if block is None:
                    block = jnp.zeros((depth, 128), F32)
                row = (ky * spots + p) * depth if place is None else place(ky, p)
                out_ref[row : row + depth, col * 128 : col * 128 + 128] = block.astype(BF)


def column_mask(n, test):
    return jnp.where(test(lanes((n, 128), 1)), 1.0, 0.0).astype(BF)


def shifted(parts, pitch):
    inside = column_mask(parts[0].shape[0], lambda lane: lane < 128 - pitch) > 0.5
    rolled = [pltpu.roll(a, 128 - pitch, 1) for a in parts]
    return [
        jnp.where(inside, rolled[v], rolled[min(v + 1, len(parts) - 1)])
        for v in range(len(parts))
    ]


def alternate(count, produce, consume):
    produce(0, 0)

    def body(i, _):
        produce(2 * i + 1, 1)
        consume(2 * i, 0)
        produce(2 * i + 2, 0)
        consume(2 * i + 1, 1)
        return 0

    lax.fori_loop(0, (count - 1) // 2, body, 0)
    consume(count - 1, 0)


def count_tables(counts, me_t, me_d, cap, per):
    nd = counts.shape[1]
    own = counts[pl.ds(me_t, 1), :].astype(F32)
    a_row = lanes((nd, nd), 1)
    a_col = lanes((nd, nd), 0)
    wide = jnp.broadcast_to(own, (nd, nd))
    start_col = jnp.sum(jnp.where(a_row < a_col, wide, 0.0), axis=1, keepdims=True)
    count_col = jnp.sum(jnp.where(a_row == a_col, wide, 0.0), axis=1, keepdims=True)
    start_row = jnp.sum(
        jnp.where(a_col < a_row, jnp.broadcast_to(count_col, (nd, nd)), 0.0), axis=0, keepdims=True
    )
    mine = lanes((1, nd), 1) == me_d
    start = jnp.sum(jnp.where(mine, start_row, 0.0), axis=1, keepdims=True).astype(jnp.int32)
    count = jnp.sum(jnp.where(mine, own, 0.0), axis=1, keepdims=True).astype(jnp.int32)
    b, j = lanes((nd, cap), 0), lanes((nd, cap), 1)
    send = (jnp.bitwise_and(b - start - j, nd - 1) == 0) & (j < count)
    rank = (lanes((per, nd), 0) * nd + me_d).astype(F32)
    take = (start_row <= rank) & (rank < start_row + own)
    rank = (lanes((nd, per), 1) * nd + me_d).astype(F32)
    give = (start_col <= rank) & (rank < start_col + count_col)
    j, b = lanes((cap, nd), 0), lanes((cap, nd), 1)
    home = (jnp.bitwise_and(b - start - j, nd - 1) == 0) & (j < count)
    as_f32 = lambda m: jnp.where(m, 1.0, 0.0)
    return as_f32(send), as_f32(take), as_f32(give), as_f32(home)


def dot_nt(a, b):
    return lax.dot_general(a, b, (((1,), (1,)), ((), ())), preferred_element_type=F32)


def chosen_rows(a, b, turn=False):
    value, pick = (a, b.astype(BF)) if turn else (b, a.astype(BF))
    high = value.astype(BF)
    rest = value - high.astype(F32)
    middle = rest.astype(BF)
    terms = (high, middle, (rest - middle.astype(F32)).astype(BF))
    parts = [dot(t, pick) if turn else dot(pick, t) for t in terms]
    return parts[0] + parts[1] + parts[2]


class Ring:
    def __init__(self, axis, other):
        self.axis, self.size, self.me = axis, lax.axis_size(axis), lax.axis_index(axis)
        self.other = lax.axis_index(other)

    def place(self, peer):
        return (peer, self.other) if self.axis == "dp" else (self.other, peer)

    def each(self, act):
        def step(i, _):
            k = 1 + lax.rem(i + self.size * 3 // 8, self.size - 1)
            act(k, jnp.bitwise_and(self.me + k, self.size - 1))
            return 0

        lax.fori_loop(0, self.size - 1, step, 0, unroll=True)

    def copy(self, k, peer, src, dst, sems):
        return pltpu.make_async_remote_copy(
            src_ref=src, dst_ref=dst, send_sem=sems.at[0], recv_sem=sems.at[1],
            device_id=self.place(peer), device_id_type=pl.DeviceIdType.MESH,
        )


    def finish(self, ref, sems):
        others = ref.at[pl.ds(0, self.size - 1)]
        for way in range(2):
            pltpu.make_async_copy(others, others, sems.at[way]).wait()


def greet(rings):
    barrier = pltpu.get_barrier_semaphore()
    for ring in rings:
        ring.each(
            lambda k, peer, ring=ring: pl.semaphore_signal(
                barrier, inc=1, device_id=ring.place(peer), device_id_type=pl.DeviceIdType.MESH
            )
        )


def meet(rings):
    pl.semaphore_wait(pltpu.get_barrier_semaphore(), sum(ring.size - 1 for ring in rings))


def send_hidden(ring, ids, reset, hid, hall, sems):
    slots, rows = hid.shape[1], ids.shape[1]
    keep = (1 - reset[...]).astype(F32)
    pick = jnp.where(lanes((slots, rows), 0) == ids[...], 1.0, 0.0)
    hall[ring.me] = dot((hid[...] * keep).astype(BF), pick.astype(BF)).astype(BF)
    copy = lambda k, peer: ring.copy(k, peer, hall.at[ring.me], hall.at[ring.me], sems)
    ring.each(lambda k, peer: copy(k, peer).start())


def core(
    feat, dp, tp, hidden_sems, waits, tables, stores,
    ids, reset, bias, head, hid, cell, win, wrec,
    out, hout, cout,
    hall, orow, inrow, fall, hp, hin, brow, rrow, gates, sem_f, sem_g, sem_h, sem_b,
):
    per = fall.shape[1]
    share, slots = hid.shape
    rows = ids.shape[1]
    send, take, give, home = tables

    spread_rows = dot(send.astype(BF), feat)
    for b in range(dp.size):
        orow[b] = spread_rows[b : b + 1]
    inrow[dp.me] = orow[dp.me]
    row_copy = lambda k, peer: dp.copy(k, peer, orow.at[peer], inrow.at[dp.me], sem_f)
    dp.each(lambda k, peer: row_copy(k, peer).start())

    waits()
    keep = (1 - reset[...]).astype(F32)
    pick = jnp.where(lanes((slots, rows), 0) == ids[...], 1.0, 0.0)
    tp.finish(hall, hidden_sems)
    everyone = hall[...].reshape(tp.size * share, rows)
    recurrent = []
    for q in range(4):
        tall = jnp.transpose(jnp.broadcast_to(bias[q : q + 1, :], (8, share)))[:, 0:1]
        gates[q * share : (q + 1) * share] = dot(wrec[q * share : (q + 1) * share], everyone) + tall
    prev_cell = chosen_rows(cell[...] * keep, pick, True)

    dp.finish(inrow, sem_f)
    gathered = jnp.concatenate([inrow[a] for a in range(dp.size)], axis=0)
    fall[tp.me] = dot(take.astype(BF), gathered.astype(BF)).astype(BF)
    feat_copy = lambda k, peer: tp.copy(k, peer, fall.at[tp.me], fall.at[tp.me], sem_g)
    tp.each(lambda k, peer: feat_copy(k, peer).start())
    tp.finish(fall, sem_g)

    features = fall[...].reshape(rows, fall.shape[2])
    sums = gates[...] + dot_nt(win[...], features)
    gate = [sums[q * share : (q + 1) * share] for q in range(4)]
    next_cell = jax.nn.sigmoid(gate[1]) * prev_cell + jax.nn.sigmoid(gate[0]) * jnp.tanh(gate[2])
    next_hidden = jax.nn.sigmoid(gate[3]) * jnp.tanh(next_cell)
    partial = jnp.transpose(dot(head[...], next_hidden.astype(BF)))
    width = partial.shape[1]
    for t in range(tp.size):
        hp[t, :, 0:width] = partial[t * per : (t + 1) * per]
    hin[tp.me] = hp[tp.me]
    sum_copy = lambda k, peer: tp.copy(k, peer, hp.at[peer], hin.at[tp.me], sem_h)
    tp.each(lambda k, peer: sum_copy(k, peer).start())

    square = lanes((rows, rows), 0) == lanes((rows, rows), 1)
    column = jnp.sum(jnp.where(square, ids[...], 0).astype(F32), axis=1, keepdims=True)
    lay = jnp.where(lanes((rows, slots), 1).astype(F32) == column, 1.0, 0.0)
    chosen = jnp.sum(lay, axis=0, keepdims=True) > 0.0
    hout[...] = jnp.where(chosen, chosen_rows(next_hidden, lay, True), hid[...])
    cout[...] = jnp.where(chosen, chosen_rows(next_cell, lay, True), cell[...])

    for store in stores:
        store.start()
    tp.finish(hin, sem_h)
    total = hin[0]
    for t in range(1, tp.size):
        total = total + hin[t]
    back = chosen_rows(give, total)
    for a in range(dp.size):
        brow[a] = back[a : a + 1]
    rrow[dp.me] = brow[dp.me]
    back_copy = lambda k, peer: dp.copy(k, peer, brow.at[peer], rrow.at[dp.me], sem_b)
    dp.each(lambda k, peer: back_copy(k, peer).start())
    dp.finish(rrow, sem_b)
    heads = chosen_rows(home, jnp.concatenate([rrow[a] for a in range(dp.size)], axis=0))
    out[...] = jnp.transpose(heads)[0 : out.shape[0], :]
    for store in stores:
        store.wait()


def encoder(
    fetch, ready, after_cut, w1, w2, w3, r1, r2, pt,
    raw, flat, sel, k1, k2, k3, kr1, kr2, ptf, ptk, u, carry, p1, p2, p3, p3r, q1,
    wide0, wide1, acc0, acc1, third,
):
    pairs, n = raw.shape[0:2]
    wide, acc = (wide0, wide1), (acc0, acc1)
    ready("conv")
    column = lanes((256, 384), 1)
    window, spot = column // 64, column % 64
    source = spot // 18 * 128 + window * 16 - 11 + spot % 18
    x = lanes((256, 384), 0)
    inside = (spot < 36) & (source // 128 == spot // 18) & (source >= 0)
    sel[...] = jnp.where(inside & (source == x), 1.0, 0.0).astype(BF)
    t1 = [spread(w1[k // 3, k % 3], 16) for k in range(9)]
    t1 = [jnp.concatenate([t, t], axis=1) for t in t1]
    row = lanes((128, 256), 0)
    spot = row % 40
    kx = spot % 18 - 2 * (lanes((128, 256), 1) // 16 % 8) - lanes((128, 256), 1) // 128
    code = jnp.where((kx >= 0) & (kx <= 2) & (spot < 36), row // 40 * 6 + spot // 18 * 3 + kx, -1)
    for pair in range(2):
        block = jnp.zeros((128, 256), F32)
        for ky in range(3):
            for c in range(2):
                for k in range(3):
                    line = t1[ky * 3 + k][pair * 2 + c : pair * 2 + c + 1]
                    block = jnp.where(code == ky * 6 + c * 3 + k, line, block)
        block = block.astype(BF)
        k1[0, pair * 128 : pair * 128 + 128] = block
        k1[1, pair * 128 : pair * 128 + 64] = block[64:]
        k1[1, pair * 128 + 64 : pair * 128 + 128] = block[:64]
    both = lambda col, i: 2 * i + col
    tail = lambda ky, p: ky * 128 + p * 16 if p < 8 else 384 + ky * 32 + (p - 8) * 16
    band_weights(k2, spread(w2[...], 32), 16, 10, 4, 2, both, tail)
    k2[480:512] = jnp.zeros((32, 256), BF)
    band_weights(k3, spread_turned(w3), 32, 12, 4, 2, both)
    same = lambda col, i: None if col * 4 + i > 10 else col * 4 + i - 1
    band_weights(kr1, spread_turned(r1), 32, 12, 4, 3, same)
    band_weights(kr2, spread_turned(r2), 32, 12, 4, 3, same)

    for r in range(3):
        for y in (0, 2 * pairs + 1, 2 * pairs + 2):
            u[r, y] = jnp.zeros((2, n, 384), BF)
    for r in range(3):
        for y in (0, 43, 44):
            p1[r, y] = jnp.zeros((n, 896), BF)
    p2[0, 0] = jnp.zeros((n, 896), BF)
    p2[0, 22] = jnp.zeros((n, 896), BF)
    p2[0, 23] = jnp.zeros((n, 896), BF)
    for ref in (p3r, q1):
        ref[0] = jnp.zeros((n, 384), BF)
        ref[12] = jnp.zeros((n, 384), BF)
    flat[...] = jnp.zeros_like(flat)

    batch = 6

    def unpack(i, slot):
        for g in range(batch):
            q = i * batch + g
            fetch(q).wait()
            flat[slot, g, :, 0:84] = raw[q].astype(F32).reshape(n * 8, 84)
        for g in range(batch):
            for y in range(2):
                for c in range(4):
                    line = ((c // 2 * batch + g) * 2 + y) * n
                    wide[slot][line : line + n, c % 2 * 128 : c % 2 * 128 + 128] = flat[
                        slot, g, pl.ds(y * 4 + c, n, stride=8), :
                    ].astype(BF)

    def cut(i, slot):
        got = dot(wide[slot][...], sel[...]).astype(BF)
        size = 2 * batch * n
        for pair in range(2):
            for v in range(3):
                part = got[pair * size : pair * size + size, v * 128 : v * 128 + 128]
                for r in range(3):
                    moved = pltpu.roll(part, 40 * r, 1) if r else part
                    u[r, pl.ds(i * 2 * batch + 1, 2 * batch), pair, :, v * 128 : v * 128 + 128] = (
                        moved.reshape(2 * batch, n, 128)
                    )

    alternate(pairs // batch, unpack, cut)
    after_cut()

    lane_in = lambda a, b: column_mask(n, lambda lane: (lane >= a) & (lane < b)) > 0.5
    ranges = (
        (lane_in(0, 40), lane_in(40, 80)),
        (lane_in(64, 104), column_mask(n, lambda lane: (lane >= 104) | (lane < 16)) > 0.5),
    )

    def first_conv(target, y, rows):
        lhs = ([], [])
        for r in range(rows):
            for v in range(3):
                packed = ([], [])
                for pair in range(2):
                    a, b, c = (
                        u[ky, y + r + ky, pair, :, v * 128 : v * 128 + 128] for ky in range(3)
                    )
                    for odd in range(2):
                        at_a, at_b = ranges[odd]
                        packed[odd].append(jnp.where(at_a, a, jnp.where(at_b, b, c)))
                for odd in range(2):
                    lhs[odd].append(jnp.concatenate(packed[odd], axis=1))
        for odd in range(2):
            got = dot(jnp.concatenate(lhs[odd], axis=0), k1[odd]).astype(BF)
            for r in range(rows):
                for v in range(3):
                    line = (r * 6 + 2 * v + odd) * n
                    target[line : line + n] = got[(r * 3 + v) * n : (r * 3 + v + 1) * n]

    def conv_row(src, y, count, step, width):
        taps = [src[y + ky] for ky in range(3)]
        return [
            jnp.concatenate([t[:, v * step : v * step + width] for t in taps], axis=1)
            for v in range(count)
        ]

    def conv_rows(src, y, rows, count, step, width, weights):
        lhs = [a for r in range(rows) for a in conv_row(src, y + r, count, step, width)]
        return dot(jnp.concatenate(lhs, axis=0), weights[...]).astype(BF)

    zero = jnp.zeros((), BF)

    end_a, end_b = lane_in(0, 32), lane_in(32, 64)

    def second_conv(target, y, rows):
        lhs = []
        for r in range(rows):
            for v in range(6):
                here, after = v * 128, v * 128 + 128
                main = [p1[0, y + r + ky, :, here : here + 128] for ky in range(3)]
                a, b, c = (p1[ky, y + r + ky, :, after : after + 128] for ky in range(3))
                ends = jnp.where(end_a, a, jnp.where(end_b, b, c))
                lhs.append(jnp.concatenate(main + [ends], axis=1))
        target[0 : rows * 6 * n] = dot(jnp.concatenate(lhs, axis=0), k2[...]).astype(BF)

    def pool_stage(conv, dst, group, count, per, pitch, offset, limit, last, copies):
        size = count * n
        conv(carry, 0, 1)
        first = column_mask(n, lambda lane: lane // pitch >= offset) > 0.5
        final = column_mask(
            n, lambda lane: lane // pitch + ((count - 1) * per - offset) < limit
        ) > 0.5

        def produce(i, slot):
            conv(acc[slot], 2 * group * i + 1, 2 * group)

        def consume(i, slot):
            for g in range(group):
                y = i * group + g
                row = lambda r, v, h: acc[slot][
                    r * size + v * n : r * size + v * n + n, h * 128 : h * 128 + 128
                ]
                keep = jnp.where(y < last, 1.0, 0.0).astype(BF) if g == group - 1 else None
                half = []
                for h in range(2):
                    tops = []
                    for v in range(count):
                        now, later = row(2 * g, v, h), row(2 * g + 1, v, h)
                        if keep is not None:
                            later = later * keep
                        if g == 0:
                            before = carry[v * n : v * n + n, h * 128 : h * 128 + 128]
                        else:
                            before = row(2 * g - 1, v, h)
                        tops.append(jnp.maximum(jnp.maximum(before, now), jnp.maximum(later, zero)))
                        if g == group - 1:
                            carry[v * n : v * n + n, h * 128 : h * 128 + 128] = later
                    half.append(tops)
                even, odd = half
                even[-1] = jnp.where(final, even[-1], zero)
                nxt = shifted(even, pitch)
                for v in range(count):
                    best = jnp.maximum(jnp.maximum(even[v], odd[v]), nxt[v])
                    if v == 0:
                        best = jnp.where(first, best, zero)
                    if v == count - 1:
                        best = jnp.where(final, best, zero)
                    for r in range(copies):
                        moved = pltpu.roll(best, 32 * r, 1) if r else best
                        dst[r, y + 1, :, v * 128 : v * 128 + 128] = moved
                for r in range(copies):
                    dst[r, y + 1, :, count * 128 : count * 128 + 128] = jnp.zeros((n, 128), BF)

        alternate((last + 1) // group, produce, consume)

    pool_stage(first_conv, p1, 6, 6, 8, 16, 5, 42, 41, 3)

    ready("dense")

    def widen(i, _):
        rows = pl.ds(i * 352, 352)
        block = pt[rows, :].astype(F32)
        ptf[0, rows, :] = block[:, :128]
        ptf[1, rows, :] = block[:, 128:]
        return 0

    lax.fori_loop(0, 11, widen, 0)

    def reorder(y, _):
        for px in range(11):
            rows = pl.ds(y * 384 + px * 32, 32)
            for h in range(2):
                ptk[rows, h * 128 : h * 128 + 128] = ptf[
                    h, pl.ds(y * 11 + px, 32, stride=121), :
                ].astype(BF)
        ptk[pl.ds(y * 384 + 352, 32), :] = jnp.zeros((32, 256), BF)
        return 0

    lax.fori_loop(0, 11, reorder, 0)

    pool_stage(second_conv, p2, 3, 6, 4, 32, 2, 21, 20, 1)

    for y in range(0, 21, 7):
        third[y * 3 * n : (y + 7) * 3 * n] = conv_rows(p2.at[0], y, 7, 3, 256, 384, k3)
    low = jnp.full((), NEG, BF)
    begin = column_mask(n, lambda lane: lane >= 32) > 0.5
    inner = column_mask(n, lambda lane: lane < 96) > 0.5
    for y in range(11):
        half = []
        for h in range(2):
            tops = []
            for v in range(3):
                top = None
                for r in range(max(2 * y - 1, 0), min(2 * y + 2, 21)):
                    at = (r * 3 + v) * n
                    part = third[at : at + n, h * 128 : h * 128 + 128]
                    top = part if top is None else jnp.maximum(top, part)
                tops.append(top)
            half.append(tops)
        even, odd = half
        even[0] = jnp.where(begin, even[0], low)
        even[2] = jnp.where(inner, even[2], low)
        nxt = shifted(even, 32)
        for v in range(3):
            best = jnp.maximum(jnp.maximum(even[v], odd[v]), nxt[v])
            if v == 2:
                best = jnp.where(inner, best, zero)
            p3[y, :, v * 128 : v * 128 + 128] = best
            p3r[y + 1, :, v * 128 : v * 128 + 128] = jnp.maximum(best, zero)

    def full_rows(src):
        return jnp.concatenate(
            [jnp.concatenate([src[y + ky] for ky in range(3)], axis=1) for y in range(11)], axis=0
        )

    q1[1:12] = jnp.maximum(dot(full_rows(p3r), kr1[...]), 0.0).astype(BF).reshape(11, n, 384)
    final = dot(full_rows(q1), kr2[...]) + p3[...].reshape(11 * n, 384).astype(F32)
    final = jnp.maximum(final, 0.0).astype(BF)
    line = jnp.concatenate([final[y * n : y * n + n] for y in range(11)], axis=1)
    return jnp.maximum(dot(line, ptk[...]), 0.0).astype(BF)


def step(*refs):
    hbm, (out, hout, cout) = refs[:16], refs[16:19]
    held, (raw, *enc), own = refs[19:34], refs[34:34 + 22], refs[34 + 22:46 + 22]
    hnew, cnew, hall, sem_q, sem_w, sem_x, sem_o = refs[46 + 22:]
    dp, tp = Ring("dp", "tensor"), Ring("tensor", "dp")
    frames = hbm[0]
    loads = [pltpu.make_async_copy(hbm[i + 1], held[i], sem_w.at[i]) for i in range(15)]
    names = ("pt", "hid", "cell", "win", "wrec", "w1", "w2", "w3", "r1", "r2")
    at = {name: i for i, name in enumerate(names + ("counts", "ids", "reset", "bias", "head"))}
    ref = lambda *which: [held[at[name]] for name in which]
    groups = {
        "conv": ("w1", "w2", "w3", "r1", "r2"),
        "dense": ("pt",),
        "hidden": ("hid", "counts", "ids", "reset"),
        "rest": ("cell", "win", "wrec", "bias", "head"),
    }

    def ready(group):
        for name in groups[group]:
            loads[at[name]].wait()

    def fetch(q):
        return pltpu.make_async_copy(frames.at[:, q], raw.at[q], sem_q.at[q])

    def start(q, _):
        fetch(q).start()
        return 0

    for name in groups["conv"] + groups["hidden"]:
        loads[at[name]].start()
    lax.fori_loop(0, raw.shape[0], start, 0)
    greet((dp, tp))
    own[4][...] = jnp.zeros_like(own[4])
    sent = []
    counts, ids, reset, hid = ref("counts", "ids", "reset", "hid")

    def share_hidden():
        for name in groups["dense"] + groups["rest"]:
            loads[at[name]].start()
        ready("hidden")
        sent.extend(count_tables(counts, tp.me, dp.me, frames.shape[0], own[2].shape[1]))
        meet((dp, tp))
        send_hidden(tp, ids, reset, hid, hall, sem_x)

    feat = encoder(fetch, ready, share_hidden, *ref(*groups["conv"], "pt"), raw, *enc)
    stores = [
        pltpu.make_async_copy(hnew, hout, sem_o.at[0]),
        pltpu.make_async_copy(cnew, cout, sem_o.at[1]),
    ]
    core(
        feat, dp, tp, sem_x, lambda: ready("rest"), sent[0:4], stores, ids, reset,
        *ref("bias", "head", "hid", "cell", "win", "wrec"), out, hnew, cnew, hall, *own,
    )


def hand_over(*refs):
    given, results, held, sems = refs[0:3], refs[3:6], refs[6:9], refs[9]
    half = held[1].shape[0] // 2
    spans = [(0, pl.ds(0, held[0].shape[0]))]
    spans += [(i, pl.ds(k * half, half)) for k in range(2) for i in (1, 2)]
    moves = [
        [
            pltpu.make_async_copy(src[i].at[rows], dst[i].at[rows], sems.at[way, at])
            for way, (src, dst) in enumerate(((given, held), (held, results)))
        ]
        for at, (i, rows) in enumerate(spans)
    ]
    for inward, _ in moves:
        inward.start()
    for inward, outward in moves:
        inward.wait()
        outward.start()
    for _, outward in moves:
        outward.wait()


def body(
    frames, counts, slot_ids, reset_flags, hidden_state, cell_state, conv_first, conv_second,
    conv_third, res_first, res_second, projection, input_weight, recur_weight, gate_bias, head_weight,
):
    n = frames.shape[0]
    share, slots = hidden_state.shape
    nd, nt = lax.axis_size("dp"), lax.axis_size("tensor")
    rows = slot_ids.shape[1]
    per = rows // nt
    width = input_weight.shape[2]
    vm = lambda *s: pltpu.VMEM(s, BF)
    vmf = lambda *s: pltpu.VMEM(s, F32)
    pair = pltpu.SemaphoreType.DMA((2,))
    anywhere = pl.BlockSpec(memory_space=pl.ANY)
    local = pl.BlockSpec(memory_space=pltpu.VMEM)
    turned = lambda w: w.transpose(2, 3, 0, 1).reshape(-1, w.shape[1])
    operands = [
        frames.transpose(0, 2, 1, 3).reshape(n, 42, 8, 84),
        projection.T, hidden_state, cell_state, input_weight.reshape(4 * share, width),
        recur_weight.reshape(4 * share, nt * share), conv_first.transpose(2, 3, 1, 0),
        conv_second.transpose(2, 3, 1, 0).reshape(144, 32), turned(conv_third), turned(res_first),
        turned(res_second), counts, slot_ids, reset_flags, gate_bias, head_weight,
    ]
    shapes = [
        jax.ShapeDtypeStruct((head_weight.shape[0], n), F32),
        jax.ShapeDtypeStruct((share, slots), F32),
        jax.ShapeDtypeStruct((share, slots), F32),
    ]
    results = pl.pallas_call(
        step,
        out_shape=shapes,
        in_specs=[anywhere] * 16,
        out_specs=[local, anywhere, anywhere],
        scratch_shapes=[pltpu.VMEM(a.shape, a.dtype) for a in operands[1:]] + [
            vm(42, n, 8, 84),
            vmf(2, 6, n * 8, 128), vm(256, 384), vm(2, 256, 256), vm(512, 256),
            vm(1152, 256), vm(1152, 384), vm(1152, 384), vmf(2, 3872, 128), vm(4224, 256),
            vm(3, 87, 2, n, 384), vm(6 * n, 256), vm(3, 45, n, 896), vm(1, 24, n, 896),
            vm(11, n, 384), vm(13, n, 384), vm(13, n, 384),
            vm(24 * n, 256), vm(24 * n, 256), vm(72 * n, 256), vm(72 * n, 256), vm(63 * n, 256),
            vmf(nd, 1, width), vmf(nd, 1, width), vm(nt, per, width), vmf(nt, per, 128),
            vmf(nt, per, 128), vmf(nd, 1, 128), vmf(nd, 1, 128), vmf(4 * share, rows),
            pair, pair, pair, pair,
            vmf(share, slots), vmf(share, slots), vm(nt, share, rows),
            pltpu.SemaphoreType.DMA((42,)), pltpu.SemaphoreType.DMA((15,)), pair, pair,
        ],
        compiler_params=pltpu.CompilerParams(
            vmem_limit_bytes=60 * 1024 * 1024, collective_id=0, has_side_effects=True
        ),
    )(*operands)
    return pl.pallas_call(
        hand_over,
        out_shape=shapes,
        in_specs=[anywhere] * 3,
        out_specs=[anywhere] * 3,
        scratch_shapes=[pltpu.VMEM(a.shape, a.dtype) for a in shapes]
        + [pltpu.SemaphoreType.DMA((2, 5))],
    )(*results)


def solution(mesh):
    return jax.shard_map(
        body,
        mesh=mesh,
        in_specs=(
            P(("dp", "tensor"), None, None, None),
            P(),
            P("dp", None),
            P("dp", None),
            P("tensor", "dp"),
            P("tensor", "dp"),
            P(),
            P(),
            P(),
            P(),
            P(),
            P(),
            P(None, "tensor", None),
            P(None, "tensor", None),
            P(None, "tensor"),
            P(None, "tensor"),
        ),
        out_specs=(P(None, ("dp", "tensor")), P("tensor", "dp"), P("tensor", "dp")),
        check_vma=False,
    )
```
